768 devices in a mesh: dp: 24 (over z, x_hi), seq: 32 (over y, x_lo, core).
Axes of the slice: x: 4 (x_hi: 2, x_lo: 2; x = x_hi * 2 + x_lo), y: 8, z: 12, core: 2. Of those that a mesh axis runs over, the one named last changes fastest.
Arguments:
- projections: bfloat16 [1, 24, 4096, 4096], P(None, 'dp', 'seq'), may hold values from -6 to 6
- rotated_query_gradient: bfloat16 [1, 24, 4096, 4096], P(None, 'dp', None, 'seq'), may hold values from -6 to 6
- gains: float32 [1, 4096], replicated, may hold values from 0.25 to 1.75
- adapter_lowering: bfloat16 [1, 48, 5120], P(None, 'dp'), may hold values from -0.078125 to 0.078125
- adapter_raising: bfloat16 [1, 48, 4096], P(None, 'dp'), may hold values from -0.875 to 0.875
- activations: bfloat16 [24, 4096, 5120], P('dp', 'seq'), may hold values from -6 to 6
- positions: int32 [3, 24, 4096], P(None, 'dp', 'seq'), may hold values from 0 to 38, as said below
- valid: int32 [24, 4096], P('dp', 'seq'), may hold values from 0 to 1, as said below
Outputs:
- grad_down: float32 [1, 48, 5120], P(None, 'dp')
- grad_up: float32 [1, 48, 4096], P(None, 'dp')
- grad_gain: float32 [1, 4096], replicated
The draws below stay inside these ranges and needn't reach their ends.
Inputs may be any that keep to these rules, and one draw needn't show every extreme that they name: `positions`: within a video the frame index never falls; one frame holds 128 tokens. Every eighth token of a video is valid.
All inputs are finite; a program needn't handle non-finite values.
Results may differ from the reference program's by a relative error of at most 0.0041.
Values may be sent and summed in bfloat16 or wider, within the bound.
No kernel may reach another device: no remote copies, remote signals or barrier semaphores. Data moves between devices by JAX's collectives and lax.ppermute only.
A program may use at most 32 MiB of HBM per device.

```python
import jax
import jax.numpy as jnp
from jax import lax

MODEL_WIDTH = 5120
HD = 128
ADAPTER_RANK = 48
QUERY_FEATURES = 4096
LEN = 4096
SAMPLES = 24


def draw_positions(key, part):
    token_index = jnp.arange(LEN, dtype=jnp.int32)
    offsets = jax.random.randint(key, (3, SAMPLES, 1), 0, 8)
    sample_index = jnp.arange(SAMPLES, dtype=jnp.int32)[None, :, None]
    offsets = jnp.where(sample_index == 0, 0, offsets)
    offsets = jnp.where(sample_index == SAMPLES - 1, 7, offsets)
    grid_base = jnp.stack([token_index // 128, token_index // 16 % 8, token_index % 16])[:, None, :]
    return (grid_base + offsets).astype(jnp.int32)


def draw_valid(key, part):
    token_index = jnp.arange(LEN, dtype=jnp.int32)
    draw_level = jax.random.randint(key, (SAMPLES, LEN), 0, 1000)
    kept_rows = draw_level < 300 + 600 * token_index // LEN
    return jnp.where((token_index % 8 == 0) | kept_rows, 1, 0).astype(jnp.int32)


def levels(rng, extent, shards, least, largest):
    gain = 1.0
    for dim, blocks in shards:
        heights = jax.random.uniform(jax.random.fold_in(jax.random.fold_in(rng, 6), dim), (blocks,), jnp.float32, least / len(shards), largest / len(shards))
        gain = gain * jnp.repeat(jnp.exp(heights), extent[dim] // blocks).reshape((-1,) + (1,) * (len(extent) - 1 - dim))
    return gain


def noise(key, dims, spread, bound, cuts=(), held_as=jnp.bfloat16):
    values = jax.random.normal(key, dims, jnp.float32) * spread
    if len(cuts) > 0:
        values = levels(key, dims, cuts, -0.22, 0.18) * values
    return jnp.clip(values, min=-bound, max=bound).astype(held_as)


def setup_inputs(seed: int = 0) -> dict:
    seeds = jax.random.split(jax.random.key(seed), 9)
    projections = noise(seeds[0], (1, SAMPLES, LEN, QUERY_FEATURES), 1.0, 6.0, ((1, 24), (2, 32)))
    rotated_query_gradient = noise(seeds[1], (1, SAMPLES, LEN, QUERY_FEATURES), 1.0, 6.0, ((1, 24), (3, 32)))
    gains = jnp.clip(1.0 + 0.15 * jax.random.normal(seeds[2], (1, QUERY_FEATURES), jnp.float32), 0.25, 1.75)
    adapter_lowering = noise(seeds[3], (1, ADAPTER_RANK, MODEL_WIDTH), MODEL_WIDTH ** -0.5, 0.078125, ((1, 24),))
    adapter_raising = noise(seeds[4], (1, ADAPTER_RANK, QUERY_FEATURES), ADAPTER_RANK ** -0.5, 0.875, ((1, 24),))
    activations = noise(seeds[5], (SAMPLES, LEN, MODEL_WIDTH), 1.0, 6.0, ((0, 24), (1, 32)))
    positions = draw_positions(jax.random.fold_in(seeds[8], 71), 0)
    valid = draw_valid(jax.random.fold_in(seeds[8], 71), 0)
    return {"projections": projections, "rotated_query_gradient": rotated_query_gradient, "gains": gains, "adapter_lowering": adapter_lowering, "adapter_raising": adapter_raising, "activations": activations, "positions": positions, "valid": valid}


EPSILON = 1e-06

def rope_tables(positions, head_size):
    one_sixth = head_size // 6
    counts = (head_size // 2 - 2 * one_sixth, one_sixth, one_sixth)
    pieces = []
    for component in range(3):
        frequency = 10000.0 ** (-jnp.arange(counts[component], dtype=jnp.float32) / counts[component])
        pieces.append(positions[component].astype(jnp.float32)[..., None] * frequency)
    angles = jnp.concatenate(pieces, -1)
    return (jnp.cos(angles), jnp.sin(angles))

def norm_backward(projections, rotated_query_gradient, gains, positions, valid):
    cosine, sine_table = rope_tables(positions, HD)
    full_shape = rotated_query_gradient.shape
    cotangent = rotated_query_gradient.astype(jnp.float32) * valid.astype(jnp.float32)[None, :, :, None]
    cotangent = cotangent.reshape(full_shape[:3] + (full_shape[3] // HD, HD // 2, 2))
    cosine = cosine[None, :, :, None, :]
    sine_table = sine_table[None, :, :, None, :]
    even_part = cosine * cotangent[..., 0] + sine_table * cotangent[..., 1]
    odd_part = cosine * cotangent[..., 1] - sine_table * cotangent[..., 0]
    unrotated = jnp.stack([even_part, odd_part], -1).reshape(full_shape)
    values = projections.astype(jnp.float32)
    inverse = lax.rsqrt(lax.optimization_barrier(jnp.mean(values * values, -1, keepdims=True)) + EPSILON)
    normed = values * inverse
    gain_part = lax.optimization_barrier(jnp.sum(unrotated * normed, axis=(1, 2)))
    scaled = unrotated * gains[:, None, None, :]
    projection_change = inverse * (scaled - normed * lax.optimization_barrier(jnp.mean(scaled * normed, -1, keepdims=True)))
    return (projection_change.astype(jnp.bfloat16), gain_part)

def adapter_partial_terms(projection_change, input_list, lowering_matrices, raising_matrices):
    down_terms = []
    up_terms = []
    for member in range(projection_change.shape[0]):
        reduced = jnp.dot(input_list, lowering_matrices[member].T, preferred_element_type=jnp.float32).astype(jnp.bfloat16)
        up_terms.append(jnp.dot(reduced.T, projection_change[member], preferred_element_type=jnp.float32))
        back_rank = jnp.dot(projection_change[member], raising_matrices[member].T, preferred_element_type=jnp.float32).astype(jnp.bfloat16)
        down_terms.append(jnp.dot(back_rank.T, input_list, preferred_element_type=jnp.float32))
    return (jnp.stack(down_terms), jnp.stack(up_terms))

def reference(projections, rotated_query_gradient, gains, adapter_lowering, adapter_raising, activations, positions, valid):
    count = jnp.sum(valid.astype(jnp.float32))
    factor = SAMPLES * LEN / count

    def one_sample(items):
        proj_one, grad_one, pos_one, valid_one, single_input = items
        projection_change, gain_part = norm_backward(proj_one[:, None], grad_one[:, None], gains, pos_one[:, None], valid_one[None])
        lowering_portion, raising_portion = adapter_partial_terms(projection_change[:, 0], single_input, adapter_lowering, adapter_raising)
        return (lowering_portion, raising_portion, gain_part)
    down_all, up_all, gain_all = lax.map(one_sample, (jnp.moveaxis(projections, 1, 0), jnp.moveaxis(rotated_query_gradient, 1, 0), jnp.moveaxis(positions, 1, 0), valid, activations))
    return (factor * lax.optimization_barrier(jnp.sum(down_all, 0)), factor * lax.optimization_barrier(jnp.sum(up_all, 0)), factor * lax.optimization_barrier(jnp.sum(gain_all, 0)))
```

```python
import jax
import jax.numpy as jnp
import numpy as np
from jax import lax
from jax.experimental import pallas as pl
from jax.experimental.pallas import tpu as pltpu
from jax.sharding import PartitionSpec as P

HD = 128
EPSILON = 1e-06
F32 = jnp.float32
BF16 = jnp.bfloat16

REM = 16


def onto(shape, dim):
    return lax.broadcasted_iota(jnp.int32, shape, dim)


def nt(a, b):
    return lax.dot_general(a, b, (((1,), (1,)), ((), ())), preferred_element_type=F32)


def nn(a, b):
    return lax.dot_general(a, b, (((1,), (0,)), ((), ())), preferred_element_type=F32)


def rope_tables(positions, valid):
    one_sixth = HD // 6
    counts = (HD // 2 - 2 * one_sixth, one_sixth, one_sixth)
    group = np.repeat(np.concatenate([np.full(n, k) for k, n in enumerate(counts)]), 2)
    powers = np.concatenate([-np.arange(n) / n for n in counts])
    frequency = np.repeat((10000.0**powers).astype(np.float32), 2)
    sign = np.where(np.arange(HD) % 2 == 0, 1.0, -1.0).astype(np.float32)
    at = positions.astype(F32)
    index = jnp.where(group == 0, at[0][:, None], jnp.where(group == 1, at[1][:, None], at[2][:, None]))
    angles = index * frequency
    keep = valid.astype(F32)[:, None]
    return jnp.cos(angles) * keep, jnp.sin(angles) * (keep * sign)


def prepare_kernel(proj, act, low, inverse, reduced):
    tokens, features = proj.shape

    def squares(h, acc):
        p = proj[:, pl.ds(pl.multiple_of(h * HD, HD), HD)].astype(F32)
        return acc + p * p

    acc = lax.fori_loop(0, features // HD, squares, jnp.zeros((tokens, HD), F32), unroll=4)
    mean = jnp.sum(acc, axis=1, keepdims=True) / features
    inverse[...] = jnp.broadcast_to(lax.rsqrt(mean + EPSILON), (tokens, HD))
    reduced[...] = nt(low[...], act[...]).astype(BF16)


def main_kernel(core, tg, proj, act, rai, inverse, reduced, cosine, sine, gains, valid, mine, theirs, scaled, delta, gain, rems):
    heads, tokens, _ = tg.shape
    features = heads * HD
    ranks = rai.shape[0]
    quarter = ranks // 4
    swap = (onto((HD, HD), 0) == (onto((HD, HD), 1) ^ 1)).astype(F32).astype(BF16)

    def first(h, acc):
        at = pl.ds(pl.multiple_of(h * HD, HD), HD)
        g = tg[h]
        unrotated = cosine[...] * g.astype(F32) + sine[...] * nn(g, swap)
        t = unrotated * (proj[:, at].astype(F32) * inverse[...])
        gain[h] = jnp.sum(t.reshape(tokens // 8, 8, HD), axis=0)
        gh = gains[:, at]
        scaled[h] = unrotated * gh
        return acc + t * gh

    acc = lax.fori_loop(0, heads, first, jnp.zeros((tokens, HD), F32), unroll=2)
    mean = jnp.broadcast_to(jnp.sum(acc, axis=1, keepdims=True) / features, (tokens, HD))

    def second(h, _):
        at = pl.ds(pl.multiple_of(h * HD, HD), HD)
        inv = inverse[...]
        normed = proj[:, at].astype(F32) * inv
        delta[:, at] = (inv * (scaled[h] - normed * mean)).astype(BF16)
        return 0

    lax.fori_loop(0, heads, second, 0, unroll=2)
    back = nt(rai[...], delta[...]).astype(BF16)
    for q in range(4):
        r = onto((REM, ranks), 0)
        pick = ((onto((REM, ranks), 1) == r + q * quarter) & (r < quarter)).astype(F32).astype(BF16)
        rems[q] = nn(pick, back).astype(BF16)
    up = reduced[...]
    count = jnp.sum(valid[...].astype(F32))
    c = core[0]

    def block(s, i, out):
        at = pl.ds(pl.multiple_of(s * HD, HD), HD)
        out[i, 0:ranks, :] = nn(up, delta[:, at]).astype(out.dtype)
        out[i, ranks : 2 * ranks, :] = nn(back, act[:, at]).astype(out.dtype)
        over = pl.ds(pl.multiple_of(features + (s // 4) * HD, HD), HD)
        rest = nn(rems[s % 4], act[:, over])
        row = onto((REM, HD), 0)
        g = jnp.sum(gain[s], axis=0, keepdims=True)
        rest = jnp.where(row == quarter, g, jnp.where(row == quarter + 1, count, rest))
        out[i, 2 * ranks : 2 * ranks + REM, :] = rest.astype(out.dtype)

    def pair(i, _):
        block(2 * i + c, i, mine)
        block(2 * i + 1 - c, i, theirs)
        return 0

    lax.fori_loop(0, heads // 2, pair, 0)


def spread_kernel(place, blocks, out, total, ranks, dp):
    peers, rows, _ = blocks.shape
    acc = blocks[0].astype(F32)
    for i in range(1, peers):
        acc = acc + blocks[i].astype(F32)
    total[...] = jnp.zeros_like(total)
    total[0:rows, :] = acc
    q = place[0]
    quarter = ranks // 4
    shape = (8 * dp, total.shape[0])
    r, k = onto(shape, 0), onto(shape, 1)
    j = r % 8
    at = 2 * (r // 8) + j % 2
    want = jnp.where(j < 2, at, at + ranks)
    rem = jnp.where(at // quarter == q, 2 * ranks + at % quarter, -1)
    want = jnp.where(j < 4, want, rem)
    want = jnp.where(j < 6, want, 2 * ranks + quarter + j - 6)
    pick = (k == want).astype(F32)
    out[...] = lax.dot_general(
        pick, total[...], (((1,), (0,)), ((), ())), precision=lax.Precision.HIGHEST, preferred_element_type=F32
    )


def finish_kernel(parts, down, up, gain, tokens):
    heads = parts.shape[0]
    factor = tokens / parts[0, 7:8, 0:1]
    for s in range(heads):
        b = parts[s] * factor
        up[:, s * HD : (s + 1) * HD] = b[0:2]
        down[:, s * HD : (s + 1) * HD] = b[2:4]
        gain[:, s * HD : (s + 1) * HD] = b[6:7]
    for t in range(heads // 4):
        b = parts[4 * t] + parts[4 * t + 1] + parts[4 * t + 2] + parts[4 * t + 3]
        down[:, (heads + t) * HD : (heads + t + 1) * HD] = b[4:6] * factor


VMEM = pl.BlockSpec(memory_space=pltpu.VMEM)
SMEM = pl.BlockSpec(memory_space=pltpu.SMEM)


def gather_ranks(adapter_lowering, adapter_raising, dp, seq):
    low_width = adapter_lowering.shape[2]
    own = jnp.concatenate([adapter_lowering[0], adapter_raising[0]], axis=1)
    full = lax.all_to_all(jnp.broadcast_to(own, (dp,) + own.shape), "dp", 0, 0, tiled=True)
    full = full.reshape(dp * own.shape[0], own.shape[1])
    return full[:, :low_width], full[:, low_width:]


def shards(projections, rotated_query_gradient, gains, adapter_lowering, adapter_raising, activations, positions, valid):
    dp, seq = lax.axis_size("dp"), lax.axis_size("seq")
    proj, act = projections[0, 0], activations[0]
    tokens, features = proj.shape
    ranks = dp * adapter_lowering.shape[1]
    member = lax.axis_index("seq")
    tg = rotated_query_gradient.reshape(seq, tokens, HD)
    tg = lax.all_to_all(tg, "seq", 0, 0, tiled=True)
    low, rai = gather_ranks(adapter_lowering, adapter_raising, dp, seq)
    cosine, sine = rope_tables(positions[:, 0], valid[0])
    inverse, reduced = pl.pallas_call(
        prepare_kernel,
        out_shape=(jax.ShapeDtypeStruct((tokens, HD), F32), jax.ShapeDtypeStruct((ranks, tokens), BF16)),
        in_specs=[VMEM] * 3,
        out_specs=(VMEM, VMEM),
    )(proj, act, low)
    rows = 2 * ranks + REM
    core = (member % 2).astype(jnp.int32).reshape(1)
    mine, theirs = pl.pallas_call(
        main_kernel,
        out_shape=(
            jax.ShapeDtypeStruct((seq // 2, rows, HD), F32),
            jax.ShapeDtypeStruct((seq // 2, rows, HD), BF16),
        ),
        in_specs=[SMEM] + [VMEM] * 10,
        out_specs=(VMEM, VMEM),
        scratch_shapes=[
            pltpu.VMEM((seq, tokens, HD), F32),
            pltpu.VMEM((tokens, features), BF16),
            pltpu.VMEM((seq, 8, HD), F32),
            pltpu.VMEM((4, REM, tokens), BF16),
        ],
    )(core, tg, proj, act, rai, inverse, reduced, cosine, sine, gains, valid)
    partner = lax.ppermute(theirs, "seq", [(s, s ^ 1) for s in range(seq)])
    both = (mine + partner.astype(F32)).astype(BF16)
    same_core = [[2 * i + c for i in range(seq // 2)] for c in range(2)]
    blocks = lax.all_to_all(both, "seq", 0, 0, tiled=True, axis_index_groups=same_core)
    place = (member % 4).astype(jnp.int32).reshape(1)
    rank_rows = pl.pallas_call(
        lambda *refs: spread_kernel(*refs, ranks=ranks, dp=dp),
        out_shape=jax.ShapeDtypeStruct((8 * dp, HD), F32),
        in_specs=[SMEM, VMEM],
        out_specs=VMEM,
        scratch_shapes=[pltpu.VMEM((128, HD), F32)],
    )(place, blocks)
    shares = lax.all_to_all(rank_rows.reshape(dp, 8, HD), "dp", 0, 0, tiled=True)
    share = jnp.sum(shares, axis=0)
    parts = lax.all_to_all(jnp.broadcast_to(share, (seq, 8, HD)), "seq", 0, 0, tiled=True)
    down, up, gain = pl.pallas_call(
        lambda *refs: finish_kernel(*refs, tokens=float(dp * seq * tokens)),
        out_shape=(
            jax.ShapeDtypeStruct((2, act.shape[1]), F32),
            jax.ShapeDtypeStruct((2, features), F32),
            jax.ShapeDtypeStruct((1, features), F32),
        ),
        in_specs=[VMEM],
        out_specs=(VMEM, VMEM, VMEM),
    )(parts)
    return down[None], up[None], gain


def solution(mesh):
    in_specs = (
        P(None, "dp", "seq", None),
        P(None, "dp", None, "seq"),
        P(),
        P(None, "dp", None),
        P(None, "dp", None),
        P("dp", "seq", None),
        P(None, "dp", "seq"),
        P("dp", "seq"),
    )
    out_specs = (P(None, "dp", None), P(None, "dp", None), P())
    return jax.shard_map(shards, mesh=mesh, in_specs=in_specs, out_specs=out_specs, check_vma=False)
```

```python
import jax
import jax.numpy as jnp
import numpy as np
from jax import lax
from jax.experimental import pallas as pl
from jax.experimental.pallas import tpu as pltpu
from jax.sharding import PartitionSpec as P

HD = 128
EPSILON = 1e-06
F32 = jnp.float32
BF16 = jnp.bfloat16

REM = 16


def onto(shape, dim):
    return lax.broadcasted_iota(jnp.int32, shape, dim)


def nt(a, b):
    return lax.dot_general(a, b, (((1,), (1,)), ((), ())), preferred_element_type=F32)


def nn(a, b):
    return lax.dot_general(a, b, (((1,), (0,)), ((), ())), preferred_element_type=F32)


def rope_tables(positions, valid):
    one_sixth = HD // 6
    counts = (HD // 2 - 2 * one_sixth, one_sixth, one_sixth)
    group = np.repeat(np.concatenate([np.full(n, k) for k, n in enumerate(counts)]), 2)
    powers = np.concatenate([-np.arange(n) / n for n in counts])
    frequency = np.repeat((10000.0**powers).astype(np.float32), 2)
    sign = np.where(np.arange(HD) % 2 == 0, 1.0, -1.0).astype(np.float32)
    at = positions.astype(F32)
    index = jnp.where(group == 0, at[0][:, None], jnp.where(group == 1, at[1][:, None], at[2][:, None]))
    angles = index * frequency
    keep = valid.astype(F32)[:, None]
    return jnp.cos(angles) * keep, jnp.sin(angles) * (keep * sign)


def both_orders(first, last):
    return jnp.concatenate([first, last], axis=0).astype(BF16), jnp.concatenate([last, first], axis=0).astype(BF16)


def prepare_kernel(proj, act, own, other, inverse, reduced):
    tokens, features = proj.shape

    def squares(h, acc):
        p = proj[:, pl.ds(pl.multiple_of(h * HD, HD), HD)].astype(F32)
        return acc + p * p

    acc = lax.fori_loop(0, features // HD, squares, jnp.zeros((tokens, HD), F32), unroll=4)
    mean = jnp.sum(acc, axis=1, keepdims=True) / features
    inverse[...] = jnp.broadcast_to(lax.rsqrt(mean + EPSILON), (tokens, HD))
    width = act.shape[1]
    reduced[0], reduced[1] = both_orders(nt(own[:, 0:width], act[...]), nt(other[:, 0:width], act[...]))


def main_kernel(core, tg, proj, act, own, other, inverse, reduced, cosine, sine, gains, valid, mine, theirs, scaled, delta, gain, rems):
    heads, tokens, _ = tg.shape
    features = heads * HD
    ranks = 2 * own.shape[0]
    width = act.shape[1]
    quarter = ranks // 4
    swap = (onto((HD, HD), 0) == (onto((HD, HD), 1) ^ 1)).astype(F32).astype(BF16)

    def first(h, acc):
        at = pl.ds(pl.multiple_of(h * HD, HD), HD)
        g = tg[h]
        unrotated = cosine[...] * g.astype(F32) + sine[...] * nn(g, swap)
        t = unrotated * (proj[:, at].astype(F32) * inverse[...])
        gain[h] = jnp.sum(t.reshape(tokens // 8, 8, HD), axis=0)
        gh = gains[:, at]
        scaled[h] = unrotated * gh
        return acc + t * gh

    acc = lax.fori_loop(0, heads, first, jnp.zeros((tokens, HD), F32), unroll=2)
    mean = jnp.broadcast_to(jnp.sum(acc, axis=1, keepdims=True) / features, (tokens, HD))

    def second(h, _):
        at = pl.ds(pl.multiple_of(h * HD, HD), HD)
        inv = inverse[...]
        normed = proj[:, at].astype(F32) * inv
        delta[:, at] = (inv * (scaled[h] - normed * mean)).astype(BF16)
        return 0

    lax.fori_loop(0, heads, second, 0, unroll=2)
    backs = both_orders(nt(own[:, width:], delta[...]), nt(other[:, width:], delta[...]))
    r = onto((REM, ranks), 0)
    for o in range(2):
        for q in range(4):
            pick = ((onto((REM, ranks), 1) == r + q * quarter) & (r < quarter)).astype(F32).astype(BF16)
            rems[o, q] = nn(pick, backs[o]).astype(BF16)
    count = jnp.sum(valid[...].astype(F32))
    c = core[0]

    def block(s, i, o, out):
        at = pl.ds(pl.multiple_of(s * HD, HD), HD)
        out[i, 0:ranks, :] = nn(reduced[o], delta[:, at]).astype(out.dtype)
        out[i, ranks : 2 * ranks, :] = nn(backs[o], act[:, at]).astype(out.dtype)
        over = pl.ds(pl.multiple_of(features + (s // 4) * HD, HD), HD)
        rest = nn(rems[o, s % 4], act[:, over])
        row = onto((REM, HD), 0)
        g = jnp.sum(gain[s], axis=0, keepdims=True)
        rest = jnp.where(row == quarter, g, jnp.where(row == quarter + 1, count, rest))
        out[i, 2 * ranks : 2 * ranks + REM, :] = rest.astype(out.dtype)

    def pair(i, _):
        block(2 * i + c, i, 0, mine)
        block(2 * i + 1 - c, i, 1, theirs)
        return 0

    lax.fori_loop(0, heads // 2, pair, 0)


def spread_kernel(place, blocks, out, total, ranks, dp):
    peers, rows, _ = blocks.shape
    acc = blocks[0].astype(F32)
    for i in range(1, peers):
        acc = acc + blocks[i].astype(F32)
    total[...] = jnp.zeros_like(total)
    total[0:rows, :] = acc
    q, c, z, hi = place[0], place[1], place[2], place[3]
    quarter = ranks // 4
    shape = (8 * dp, total.shape[0])
    r, k = onto(shape, 0), onto(shape, 1)
    j = r % 8
    dest = r // 8
    far = (dest // 2 - z + dp // 2) % (dp // 2)
    at = 4 * (far // 2 + dp // 4 * ((far % 2) ^ c)) + 2 * ((dest % 2) ^ hi) + j % 2
    want = jnp.where(j < 2, at, at + ranks)
    rem = jnp.where(at // quarter == q, 2 * ranks + at % quarter, -1)
    want = jnp.where(j < 4, want, rem)
    want = jnp.where(j < 6, want, 2 * ranks + quarter + j - 6)
    pick = (k == want).astype(F32)
    out[...] = lax.dot_general(
        pick, total[...], (((1,), (0,)), ((), ())), precision=lax.Precision.HIGHEST, preferred_element_type=F32
    )


def finish_kernel(parts, down, up, gain, tokens):
    heads = parts.shape[0]
    factor = tokens / parts[0, 7:8, 0:1]
    for s in range(heads):
        b = parts[s] * factor
        up[:, s * HD : (s + 1) * HD] = b[0:2]
        down[:, s * HD : (s + 1) * HD] = b[2:4]
        gain[:, s * HD : (s + 1) * HD] = b[6:7]
    for t in range(heads // 4):
        b = parts[4 * t] + parts[4 * t + 1] + parts[4 * t + 2] + parts[4 * t + 3]
        down[:, (heads + t) * HD : (heads + t + 1) * HD] = b[4:6] * factor


VMEM = pl.BlockSpec(memory_space=pltpu.VMEM)
SMEM = pl.BlockSpec(memory_space=pltpu.SMEM)


def within(mib):
    return pltpu.CompilerParams(vmem_limit_bytes=mib * 2**20)


def gather_ranks(adapter_lowering, adapter_raising, dp, seq):
    own = jnp.concatenate([adapter_lowering[0], adapter_raising[0]], axis=1)
    near = lax.ppermute(own, "dp", [(d, d ^ 1) for d in range(dp)])
    pair = jnp.concatenate([own, near], axis=0)
    length = dp // 2
    pieces = []
    for j in range(length // 2):
        moves = []
        for d in range(dp):
            for s in range(seq):
                to = 2 * ((d // 2 - (2 * j + s % 2)) % length) + d % 2
                moves.append((d * seq + s, to * seq + s))
        pieces.append(lax.ppermute(pair, ("dp", "seq"), moves))
    half = jnp.concatenate(pieces, axis=0)
    return half, lax.ppermute(half, "seq", [(s, s ^ 1) for s in range(seq)])


def shards(projections, rotated_query_gradient, gains, adapter_lowering, adapter_raising, activations, positions, valid):
    dp, seq = lax.axis_size("dp"), lax.axis_size("seq")
    proj, act = projections[0, 0], activations[0]
    tokens, features = proj.shape
    ranks = dp * adapter_lowering.shape[1]
    member = lax.axis_index("seq")
    tg = rotated_query_gradient.reshape(seq, tokens, HD)
    tg = lax.all_to_all(tg, "seq", 0, 0, tiled=True)
    own, other = gather_ranks(adapter_lowering, adapter_raising, dp, seq)
    cosine, sine = rope_tables(positions[:, 0], valid[0])
    inverse, reduced = pl.pallas_call(
        prepare_kernel,
        out_shape=(jax.ShapeDtypeStruct((tokens, HD), F32), jax.ShapeDtypeStruct((2, ranks, tokens), BF16)),
        in_specs=[VMEM] * 4,
        out_specs=(VMEM, VMEM),
        compiler_params=within(6),
    )(proj, act, own, other)
    rows = 2 * ranks + REM
    core = (member % 2).astype(jnp.int32).reshape(1)
    mine, theirs = pl.pallas_call(
        main_kernel,
        out_shape=(
            jax.ShapeDtypeStruct((seq // 2, rows, HD), F32),
            jax.ShapeDtypeStruct((seq // 2, rows, HD), BF16),
        ),
        in_specs=[SMEM] + [VMEM] * 11,
        out_specs=(VMEM, VMEM),
        compiler_params=within(12),
        scratch_shapes=[
            pltpu.VMEM((seq, tokens, HD), F32),
            pltpu.VMEM((tokens, features), BF16),
            pltpu.VMEM((seq, 8, HD), F32),
            pltpu.VMEM((2, 4, REM, tokens), BF16),
        ],
    )(core, tg, proj, act, own, other, inverse, reduced, cosine, sine, gains, valid)
    partner = lax.ppermute(theirs, "seq", [(s, s ^ 1) for s in range(seq)])
    both = (mine + partner.astype(F32)).astype(BF16)
    same_core = [[2 * i + c for i in range(seq // 2)] for c in range(2)]
    blocks = lax.all_to_all(both, "seq", 0, 0, tiled=True, axis_index_groups=same_core)
    video = lax.axis_index("dp")
    place = jnp.stack([member % 4, member % 2, video // 2, video % 2]).astype(jnp.int32)
    rank_rows = pl.pallas_call(
        lambda *refs: spread_kernel(*refs, ranks=ranks, dp=dp),
        out_shape=jax.ShapeDtypeStruct((8 * dp, HD), F32),
        in_specs=[SMEM, VMEM],
        out_specs=VMEM,
        compiler_params=within(4),
        scratch_shapes=[pltpu.VMEM((128, HD), F32)],
    )(place, blocks)
    shares = lax.all_to_all(rank_rows.reshape(dp, 8, HD), "dp", 0, 0, tiled=True)
    share = jnp.sum(shares, axis=0)
    parts = lax.all_to_all(jnp.broadcast_to(share, (seq, 8, HD)), "seq", 0, 0, tiled=True)
    down, up, gain = pl.pallas_call(
        lambda *refs: finish_kernel(*refs, tokens=float(dp * seq * tokens)),
        out_shape=(
            jax.ShapeDtypeStruct((2, act.shape[1]), F32),
            jax.ShapeDtypeStruct((2, features), F32),
            jax.ShapeDtypeStruct((1, features), F32),
        ),
        in_specs=[VMEM],
        out_specs=(VMEM, VMEM, VMEM),
        compiler_params=within(4),
    )(parts)
    return down[None], up[None], gain


def solution(mesh):
    in_specs = (
        P(None, "dp", "seq", None),
        P(None, "dp", None, "seq"),
        P(),
        P(None, "dp", None),
        P(None, "dp", None),
        P("dp", "seq", None),
        P(None, "dp", "seq"),
        P("dp", "seq"),
    )
    out_specs = (P(None, "dp", None), P(None, "dp", None), P())
    return jax.shard_map(shards, mesh=mesh, in_specs=in_specs, out_specs=out_specs, check_vma=False)
```

```python
import jax
import jax.numpy as jnp
import numpy as np
from jax import lax
from jax.experimental import pallas as pl
from jax.experimental.pallas import tpu as pltpu
from jax.sharding import PartitionSpec as P

HD = 128
EPSILON = 1e-06
F32 = jnp.float32
BF16 = jnp.bfloat16

REM = 16


def onto(shape, dim):
    return lax.broadcasted_iota(jnp.int32, shape, dim)


def nt(a, b):
    return lax.dot_general(a, b, (((1,), (1,)), ((), ())), preferred_element_type=F32)


def nn(a, b):
    return lax.dot_general(a, b, (((1,), (0,)), ((), ())), preferred_element_type=F32)


def rope_tables(positions, valid):
    one_sixth = HD // 6
    counts = (HD // 2 - 2 * one_sixth, one_sixth, one_sixth)
    group = np.repeat(np.concatenate([np.full(n, k) for k, n in enumerate(counts)]), 2)
    powers = np.concatenate([-np.arange(n) / n for n in counts])
    frequency = np.repeat((10000.0**powers).astype(np.float32), 2)
    sign = np.where(np.arange(HD) % 2 == 0, 1.0, -1.0).astype(np.float32)
    at = positions.astype(F32)
    index = jnp.where(group == 0, at[0][:, None], jnp.where(group == 1, at[1][:, None], at[2][:, None]))
    angles = index * frequency
    keep = valid.astype(F32)[:, None]
    return jnp.cos(angles) * keep, jnp.sin(angles) * (keep * sign)


def main_kernel(core, tg, proj, act, maps, cosine, sine, gains, valid, mine, theirs, scaled, delta, gain, rems):
    heads, tokens, _ = tg.shape
    features = heads * HD
    ranks = maps.shape[0]
    width = act.shape[1]
    quarter = ranks // 4

    def lanes(tile):
        return pl.ds(pl.multiple_of(tile * HD, HD), HD)

    def squares(h, acc):
        p = proj[:, lanes(h)].astype(F32)
        return acc + p * p

    acc = lax.fori_loop(0, heads, squares, jnp.zeros((tokens, HD), F32), unroll=4)
    mean = jnp.sum(acc, axis=1, keepdims=True) / features
    inverse = jnp.broadcast_to(lax.rsqrt(mean + EPSILON), (tokens, HD))
    swap = (onto((HD, HD), 0) == (onto((HD, HD), 1) ^ 1)).astype(F32).astype(BF16)

    def first(h, acc):
        g = tg[h]
        unrotated = cosine[...] * g.astype(F32) + sine[...] * nn(g, swap)
        t = unrotated * (proj[:, lanes(h)].astype(F32) * inverse)
        gain[h] = jnp.sum(t.reshape(tokens // 8, 8, HD), axis=0)
        gh = gains[:, lanes(h)]
        scaled[h] = unrotated * gh
        return acc + t * gh

    acc = lax.fori_loop(0, heads, first, jnp.zeros((tokens, HD), F32), unroll=2)
    mean = jnp.broadcast_to(jnp.sum(acc, axis=1, keepdims=True) / features, (tokens, HD))

    def second(h, _):
        normed = proj[:, lanes(h)].astype(F32) * inverse
        delta[:, lanes(h)] = (inverse * (scaled[h] - normed * mean)).astype(BF16)
        return 0

    lax.fori_loop(0, heads, second, 0, unroll=2)
    up = nt(maps[:, 0:width], act[...]).astype(BF16)
    back = nt(maps[:, width:], delta[...]).astype(BF16)
    r = onto((REM, ranks), 0)
    for q in range(4):
        pick = ((onto((REM, ranks), 1) == r + q * quarter) & (r < quarter)).astype(F32).astype(BF16)
        rems[q] = nn(pick, back).astype(BF16)
    count = jnp.sum(valid[...].astype(F32))
    c = core[0]

    def block(s, i, out):
        out[i, 0:ranks, :] = nn(up, delta[:, lanes(s)]).astype(out.dtype)
        out[i, ranks : 2 * ranks, :] = nn(back, act[:, lanes(s)]).astype(out.dtype)
        rest = nn(rems[s % 4], act[:, lanes(heads + s // 4)])
        row = onto((REM, HD), 0)
        g = jnp.sum(gain[s], axis=0, keepdims=True)
        rest = jnp.where(row == quarter, g, jnp.where(row == quarter + 1, count, rest))
        out[i, 2 * ranks : 2 * ranks + REM, :] = rest.astype(out.dtype)

    def pair(i, _):
        block(2 * i + c, i, mine)
        block(2 * i + 1 - c, i, theirs)
        return 0

    lax.fori_loop(0, heads // 2, pair, 0)


def spread_kernel(place, blocks, out, total, ranks, dp):
    peers, rows, _ = blocks.shape
    acc = blocks[0].astype(F32)
    for i in range(1, peers):
        acc = acc + blocks[i].astype(F32)
    total[...] = jnp.zeros_like(total)
    total[0:rows, :] = acc
    q, hi = place[0], place[1]
    quarter = ranks // 4
    shape = (8 * dp, total.shape[0])
    r, k = onto(shape, 0), onto(shape, 1)
    j = r % 8
    dest = r // 8
    at = 4 * (dest // 2) + 2 * ((dest % 2) ^ hi) + j % 2
    want = jnp.where(j < 2, at, at + ranks)
    rem = jnp.where(at // quarter == q, 2 * ranks + at % quarter, -1)
    want = jnp.where(j < 4, want, rem)
    want = jnp.where(j < 6, want, 2 * ranks + quarter + j - 6)
    pick = (k == want).astype(F32)
    out[...] = lax.dot_general(
        pick, total[...], (((1,), (0,)), ((), ())), precision=lax.Precision.HIGHEST, preferred_element_type=F32
    )


def finish_kernel(parts, down, up, gain, tokens):
    heads = parts.shape[0]
    factor = tokens / parts[0, 7:8, 0:1]
    for s in range(heads):
        b = parts[s] * factor
        up[:, s * HD : (s + 1) * HD] = b[0:2]
        down[:, s * HD : (s + 1) * HD] = b[2:4]
        gain[:, s * HD : (s + 1) * HD] = b[6:7]
    for t in range(heads // 4):
        b = parts[4 * t] + parts[4 * t + 1] + parts[4 * t + 2] + parts[4 * t + 3]
        down[:, (heads + t) * HD : (heads + t + 1) * HD] = b[4:6] * factor


VMEM = pl.BlockSpec(memory_space=pltpu.VMEM)
SMEM = pl.BlockSpec(memory_space=pltpu.SMEM)


def within(mib):
    return pltpu.CompilerParams(vmem_limit_bytes=mib * 2**20)


def gather_ranks(adapter_lowering, adapter_raising, dp):
    own = jnp.concatenate([adapter_lowering, adapter_raising], axis=2)
    near = lax.ppermute(own, "dp", [(d, d ^ 1) for d in range(dp)])
    pair = jnp.concatenate([own, near], axis=0)
    along_z = [list(range(hi, dp, 2)) for hi in range(2)]
    full = lax.all_gather(pair, "dp", axis=0, tiled=True, axis_index_groups=along_z)
    return full.reshape(dp * own.shape[1], own.shape[2])


def shards(projections, rotated_query_gradient, gains, adapter_lowering, adapter_raising, activations, positions, valid):
    dp, seq = lax.axis_size("dp"), lax.axis_size("seq")
    proj, act = projections[0, 0], activations[0]
    tokens, features = proj.shape
    ranks = dp * adapter_lowering.shape[1]
    member = lax.axis_index("seq")
    tg = rotated_query_gradient.reshape(seq, tokens, HD)
    tg = lax.all_to_all(tg, "seq", 0, 0, tiled=True)
    maps = gather_ranks(adapter_lowering, adapter_raising, dp)
    cosine, sine = rope_tables(positions[:, 0], valid[0])
    rows = 2 * ranks + REM
    core = (member % 2).astype(jnp.int32).reshape(1)
    mine, theirs = pl.pallas_call(
        main_kernel,
        out_shape=(
            jax.ShapeDtypeStruct((seq // 2, rows, HD), F32),
            jax.ShapeDtypeStruct((seq // 2, rows, HD), BF16),
        ),
        in_specs=[SMEM] + [VMEM] * 8,
        out_specs=(VMEM, VMEM),
        compiler_params=within(12),
        scratch_shapes=[
            pltpu.VMEM((seq, tokens, HD), F32),
            pltpu.VMEM((tokens, features), BF16),
            pltpu.VMEM((seq, 8, HD), F32),
            pltpu.VMEM((4, REM, tokens), BF16),
        ],
    )(core, tg, proj, act, maps, cosine, sine, gains, valid)
    partner = lax.ppermute(theirs, "seq", [(s, s ^ 1) for s in range(seq)])
    both = (mine + partner.astype(F32)).astype(BF16)
    same_core = [[2 * i + c for i in range(seq // 2)] for c in range(2)]
    blocks = lax.all_to_all(both, "seq", 0, 0, tiled=True, axis_index_groups=same_core)
    video = lax.axis_index("dp")
    place = jnp.stack([member % 4, video % 2]).astype(jnp.int32)
    rank_rows = pl.pallas_call(
        lambda *refs: spread_kernel(*refs, ranks=ranks, dp=dp),
        out_shape=jax.ShapeDtypeStruct((8 * dp, HD), F32),
        in_specs=[SMEM, VMEM],
        out_specs=VMEM,
        compiler_params=within(4),
        scratch_shapes=[pltpu.VMEM((128, HD), F32)],
    )(place, blocks)
    shares = lax.all_to_all(rank_rows.reshape(dp, 8, HD), "dp", 0, 0, tiled=True)
    share = jnp.sum(shares, axis=0)
    parts = lax.all_to_all(jnp.broadcast_to(share, (seq, 8, HD)), "seq", 0, 0, tiled=True)
    down, up, gain = pl.pallas_call(
        lambda *refs: finish_kernel(*refs, tokens=float(dp * seq * tokens)),
        out_shape=(
            jax.ShapeDtypeStruct((2, act.shape[1]), F32),
            jax.ShapeDtypeStruct((2, features), F32),
            jax.ShapeDtypeStruct((1, features), F32),
        ),
        in_specs=[VMEM],
        out_specs=(VMEM, VMEM, VMEM),
        compiler_params=within(4),
    )(parts)
    return down[None], up[None], gain


def solution(mesh):
    in_specs = (
        P(None, "dp", "seq", None),
        P(None, "dp", None, "seq"),
        P(),
        P(None, "dp", None),
        P(None, "dp", None),
        P("dp", "seq", None),
        P(None, "dp", "seq"),
        P("dp", "seq"),
    )
    out_specs = (P(None, "dp", None), P(None, "dp", None), P())
    return jax.shard_map(shards, mesh=mesh, in_specs=in_specs, out_specs=out_specs, check_vma=False)
```

```python
import jax
import jax.numpy as jnp
import numpy as np
from jax import lax
from jax.experimental import pallas as pl
from jax.experimental.pallas import tpu as pltpu
from jax.sharding import PartitionSpec as P


HD = 128
EPSILON = 1e-06
F32 = jnp.float32
BF16 = jnp.bfloat16

REM = 16


def onto(shape, dim):
    return lax.broadcasted_iota(jnp.int32, shape, dim)


def nt(a, b):
    return lax.dot_general(a, b, (((1,), (1,)), ((), ())), preferred_element_type=F32)


def nn(a, b):
    return lax.dot_general(a, b, (((1,), (0,)), ((), ())), preferred_element_type=F32)


def rope_tables(positions, valid):
    one_sixth = HD // 6
    counts = (HD // 2 - 2 * one_sixth, one_sixth, one_sixth)
    group = np.repeat(np.concatenate([np.full(n, k) for k, n in enumerate(counts)]), 2)
    powers = np.concatenate([-np.arange(n) / n for n in counts])
    frequency = np.repeat((10000.0**powers).astype(np.float32), 2)
    sign = np.where(np.arange(HD) % 2 == 0, 1.0, -1.0).astype(np.float32)
    at = positions.astype(F32)
    index = jnp.where(group == 0, at[0][:, None], jnp.where(group == 1, at[1][:, None], at[2][:, None]))
    angles = index * frequency
    keep = valid.astype(F32)[:, None]
    return jnp.cos(angles) * keep, jnp.sin(angles) * (keep * sign)


def main_kernel(place, tg, proj, act, half, other, cosine, sine, gains, valid, mine, theirs, *scratch):
    maps, scaled, delta, gain = scratch
    heads, tokens, _ = tg.shape
    features = heads * HD
    ranks, cut = half.shape
    width = act.shape[1]
    quarter = ranks // 4
    c = place[0]

    @pl.when(c == 0)
    def _():
        maps[:, 0:cut] = half[...]
        maps[:, cut:] = other[...]

    @pl.when(c != 0)
    def _():
        maps[:, 0:cut] = other[...]
        maps[:, cut:] = half[...]

    up = nt(maps[:, 0:width], act[...]).astype(BF16)

    def lanes(tile, count=1):
        return pl.ds(pl.multiple_of(tile * HD, HD), count * HD)

    def squares(h, acc):
        p = proj[:, lanes(h)].astype(F32)
        return acc + p * p

    acc = lax.fori_loop(0, heads, squares, jnp.zeros((tokens, HD), F32), unroll=4)
    mean = jnp.sum(acc, axis=1, keepdims=True) / features
    inverse = jnp.broadcast_to(lax.rsqrt(mean + EPSILON), (tokens, HD))
    swap = (onto((HD, HD), 0) == (onto((HD, HD), 1) ^ 1)).astype(F32).astype(BF16)

    def first(k, acc):
        g4 = tg[pl.ds(4 * k, 4)].reshape(4 * tokens, HD)
        s4 = nn(g4, swap)
        for b in range(4):
            h = 4 * k + b
            g = g4[b * tokens : (b + 1) * tokens].astype(F32)
            unrotated = cosine[...] * g + sine[...] * s4[b * tokens : (b + 1) * tokens]
            t = unrotated * (proj[:, lanes(h)].astype(F32) * inverse)
            gain[h] = jnp.sum(t.reshape(tokens // 8, 8, HD), axis=0)
            gh = gains[:, lanes(h)]
            scaled[h] = unrotated * gh
            acc = acc + t * gh
        return acc

    acc = lax.fori_loop(0, heads // 4, first, jnp.zeros((tokens, HD), F32))
    mean = jnp.broadcast_to(jnp.sum(acc, axis=1, keepdims=True) / features, (tokens, HD))

    def second(h, _):
        normed = proj[:, lanes(h)].astype(F32) * inverse
        delta[:, lanes(h)] = (inverse * (scaled[h] - normed * mean)).astype(BF16)
        return 0

    lax.fori_loop(0, heads, second, 0, unroll=4)
    back = nt(maps[:, width:], delta[...]).astype(BF16)
    r, k = onto((4 * REM, ranks), 0), onto((4 * REM, ranks), 1)
    pick = ((k == r // REM * quarter + r % REM) & (r % REM < quarter)).astype(F32).astype(BF16)
    rems = nn(pick, back).astype(BF16)
    count = jnp.sum(valid[...].astype(F32))
    row = onto((REM, HD), 0)

    def four(t, _):
        ups = nn(up, delta[:, lanes(4 * t, 4)])
        downs = nn(back, act[:, lanes(4 * t, 4)])
        rests = nn(rems, act[:, lanes(heads + t)])
        blocks = []
        for b in range(4):
            g = jnp.sum(gain[4 * t + b], axis=0, keepdims=True)
            rest = rests[b * REM : (b + 1) * REM]
            rest = jnp.where(row == quarter, g, jnp.where(row == quarter + 1, count, rest))
            at = slice(b * HD, (b + 1) * HD)
            blocks.append((ups[:, at], downs[:, at], rest))
        for p in range(2):
            i = 2 * t + p
            for j, (first_row, rows) in enumerate(((0, ranks), (ranks, ranks), (2 * ranks, REM))):
                even, odd = blocks[2 * p][j], blocks[2 * p + 1][j]
                mine[i, first_row : first_row + rows, :] = jnp.where(c == 0, even, odd)
                theirs[i, first_row : first_row + rows, :] = jnp.where(c == 0, odd, even).astype(theirs.dtype)
        return 0

    lax.fori_loop(0, heads // 4, four, 0)


def spread_kernel(place, blocks, out, total, ranks, dp):
    peers, rows, _ = blocks.shape
    acc = blocks[0].astype(F32)
    for i in range(1, peers):
        acc = acc + blocks[i].astype(F32)
    total[...] = jnp.zeros_like(total)
    total[0:rows, :] = acc
    q, hi = place[1], place[2]
    quarter = ranks // 4
    shape = (8 * dp, total.shape[0])
    r, k = onto(shape, 0), onto(shape, 1)
    j = r % 8
    dest = r // 8
    at = 4 * (dest // 2) + 2 * ((dest % 2) ^ hi) + j % 2
    want = jnp.where(j < 2, at, at + ranks)
    rem = jnp.where(at // quarter == q, 2 * ranks + at % quarter, -1)
    want = jnp.where(j < 4, want, rem)
    want = jnp.where(j < 6, want, 2 * ranks + quarter + j - 6)
    pick = (k == want).astype(F32)
    out[...] = lax.dot_general(
        pick, total[...], (((1,), (0,)), ((), ())), precision=lax.Precision.HIGHEST, preferred_element_type=F32
    )


def finish_kernel(parts, down, up, gain, tokens):
    heads = parts.shape[0]
    factor = tokens / parts[0, 7:8, 0:1]
    for s in range(heads):
        b = parts[s] * factor
        up[:, s * HD : (s + 1) * HD] = b[0:2]
        down[:, s * HD : (s + 1) * HD] = b[2:4]
        gain[:, s * HD : (s + 1) * HD] = b[6:7]
    for t in range(heads // 4):
        b = parts[4 * t] + parts[4 * t + 1] + parts[4 * t + 2] + parts[4 * t + 3]
        down[:, (heads + t) * HD : (heads + t + 1) * HD] = b[4:6] * factor


VMEM = pl.BlockSpec(memory_space=pltpu.VMEM)
SMEM = pl.BlockSpec(memory_space=pltpu.SMEM)


def within(mib):
    return pltpu.CompilerParams(vmem_limit_bytes=mib * 2**20)


def gather_ranks(adapter_lowering, adapter_raising, dp, seq, member):
    own = jnp.concatenate([adapter_lowering, adapter_raising], axis=2)
    cut = own.shape[2] // 2
    own = jnp.where(member % 2 == 0, own[:, :, :cut], own[:, :, cut:])
    near = lax.ppermute(own, "dp", [(d, d ^ 1) for d in range(dp)])
    pair = jnp.concatenate([own, near], axis=0)
    along_z = [list(range(hi, dp, 2)) for hi in range(2)]
    half = lax.all_gather(pair, "dp", axis=0, tiled=True, axis_index_groups=along_z)
    half = half.reshape(dp * own.shape[1], cut)
    return half, lax.ppermute(half, "seq", [(s, s ^ 1) for s in range(seq)])


def shards(projections, rotated_query_gradient, gains, adapter_lowering, adapter_raising, activations, positions, valid):
    dp, seq = lax.axis_size("dp"), lax.axis_size("seq")
    proj, act = projections[0, 0], activations[0]
    tokens, features = proj.shape
    ranks = dp * adapter_lowering.shape[1]
    member = lax.axis_index("seq")
    tg = rotated_query_gradient.reshape(seq, tokens, HD)
    tg = lax.all_to_all(tg, "seq", 0, 0, tiled=True)
    half, other = gather_ranks(adapter_lowering, adapter_raising, dp, seq, member)
    cosine, sine = rope_tables(positions[:, 0], valid[0])
    rows = 2 * ranks + REM
    place = jnp.stack([member % 2, member % 4, lax.axis_index("dp") % 2]).astype(jnp.int32)
    mine, theirs = pl.pallas_call(
        main_kernel,
        out_shape=(
            jax.ShapeDtypeStruct((seq // 2, rows, HD), F32),
            jax.ShapeDtypeStruct((seq // 2, rows, HD), BF16),
        ),
        in_specs=[SMEM] + [VMEM] * 9,
        out_specs=(VMEM, VMEM),
        compiler_params=within(14),
        scratch_shapes=[
            pltpu.VMEM((ranks, act.shape[1] + features), BF16),
            pltpu.VMEM((seq, tokens, HD), F32),
            pltpu.VMEM((tokens, features), BF16),
            pltpu.VMEM((seq, 8, HD), F32),
        ],
    )(place, tg, proj, act, half, other, cosine, sine, gains, valid)
    partner = lax.ppermute(theirs, "seq", [(s, s ^ 1) for s in range(seq)])
    both = (mine + partner.astype(F32)).astype(BF16)
    same_core = [[2 * i + c for i in range(seq // 2)] for c in range(2)]
    blocks = lax.all_to_all(both, "seq", 0, 0, tiled=True, axis_index_groups=same_core)
    rank_rows = pl.pallas_call(
        lambda *refs: spread_kernel(*refs, ranks=ranks, dp=dp),
        out_shape=jax.ShapeDtypeStruct((8 * dp, HD), F32),
        in_specs=[SMEM, VMEM],
        out_specs=VMEM,
        compiler_params=within(4),
        scratch_shapes=[pltpu.VMEM((128, HD), F32)],
    )(place, blocks)
    shares = lax.all_to_all(rank_rows.reshape(dp, 8, HD), "dp", 0, 0, tiled=True)
    share = jnp.sum(shares, axis=0)
    parts = lax.all_to_all(jnp.broadcast_to(share, (seq, 8, HD)), "seq", 0, 0, tiled=True)
    down, up, gain = pl.pallas_call(
        lambda *refs: finish_kernel(*refs, tokens=float(dp * seq * tokens)),
        out_shape=(
            jax.ShapeDtypeStruct((2, act.shape[1]), F32),
            jax.ShapeDtypeStruct((2, features), F32),
            jax.ShapeDtypeStruct((1, features), F32),
        ),
        in_specs=[VMEM],
        out_specs=(VMEM, VMEM, VMEM),
        compiler_params=within(4),
    )(parts)
    return down[None], up[None], gain


def solution(mesh):
    in_specs = (
        P(None, "dp", "seq", None),
        P(None, "dp", None, "seq"),
        P(),
        P(None, "dp", None),
        P(None, "dp", None),
        P("dp", "seq", None),
        P(None, "dp", "seq"),
        P("dp", "seq"),
    )
    out_specs = (P(None, "dp", None), P(None, "dp", None), P())
    return jax.shard_map(shards, mesh=mesh, in_specs=in_specs, out_specs=out_specs, check_vma=False)
```

```python
import jax
import jax.numpy as jnp
import numpy as np
from jax import lax
from jax.experimental import pallas as pl
from jax.experimental.pallas import tpu as pltpu
from jax.sharding import PartitionSpec as P


HD = 128
EPSILON = 1e-06
F32 = jnp.float32
BF16 = jnp.bfloat16

REM = 8


def onto(shape, dim):
    return lax.broadcasted_iota(jnp.int32, shape, dim)


def nt(a, b):
    return lax.dot_general(a, b, (((1,), (1,)), ((), ())), preferred_element_type=F32)


def nn(a, b):
    return lax.dot_general(a, b, (((1,), (0,)), ((), ())), preferred_element_type=F32)


def rope_tables(positions, valid):
    one_sixth = HD // 6
    counts = (HD // 2 - 2 * one_sixth, one_sixth, one_sixth)
    group = np.repeat(np.concatenate([np.full(n, k) for k, n in enumerate(counts)]), 2)
    powers = np.concatenate([-np.arange(n) / n for n in counts])
    frequency = np.repeat((10000.0**powers).astype(np.float32), 2)
    sign = np.where(np.arange(HD) % 2 == 0, 1.0, -1.0).astype(np.float32)
    at = positions.astype(F32)
    index = jnp.where(group == 0, at[0][:, None], jnp.where(group == 1, at[1][:, None], at[2][:, None]))
    angles = index * frequency
    keep = valid.astype(F32)[:, None]
    return jnp.cos(angles) * keep, jnp.sin(angles) * (keep * sign)


def delta_kernel(tg, proj, cosine, sine, gains, delta, gain, gains8):
    heads, tokens, _ = tg.shape
    features = heads * HD
    even = onto((8, HD), 1) % 2 == 0
    gain[...] = jnp.zeros_like(gain)
    gains8[...] = jnp.broadcast_to(gains[...], gains8.shape)
    group = 4

    def mean_of(parts):
        mean = jnp.sum((parts[0] + parts[1]) + (parts[2] + parts[3]), axis=1, keepdims=True) / features
        return jnp.broadcast_to(mean, (8, HD))

    def some(k, _):
        rows = [pl.ds(pl.multiple_of(8 * (group * k + b), 8), 8) for b in range(group)]
        inverse, cos8, sin8 = [], [], []
        ps = [[proj[r, h * HD : (h + 1) * HD].astype(F32) for h in range(heads)] for r in rows]
        for b, r in enumerate(rows):
            acc = [jnp.zeros((8, HD), F32)] * 4
            for h in range(heads):
                acc[h % 4] = acc[h % 4] + ps[b][h] * ps[b][h]
            inverse.append(lax.rsqrt(mean_of(acc) + EPSILON))
            cos8.append(cosine[r, :] * inverse[b])
            sin8.append(sine[r, :] * inverse[b])
        ws = [[None] * heads for _ in rows]
        acc = [[jnp.zeros((8, HD), F32)] * 4 for _ in rows]
        for h in range(heads):
            gh = gains8[:, h * HD : (h + 1) * HD]
            total = gain[h]
            for b, r in enumerate(rows):
                g = tg[h, r, :].astype(F32)
                turned = jnp.where(even, pltpu.roll(g, HD - 1, 1), pltpu.roll(g, 1, 1))
                u = cos8[b] * g + sin8[b] * turned
                p = ps[b][h]
                total = total + u * p
                ws[b][h] = u * gh
                acc[b][h % 4] = acc[b][h % 4] + ws[b][h] * p
            gain[h] = total
        for b, r in enumerate(rows):
            mean = mean_of(acc[b]) * (inverse[b] * inverse[b])
            for h in range(heads):
                delta[r, h * HD : (h + 1) * HD] = (ws[b][h] - ps[b][h] * mean).astype(BF16)
        return 0

    lax.fori_loop(0, tokens // (8 * group), some, 0, unroll=1)


def sums_kernel(place, act, half, other, delta, gain, valid, mine, theirs, maps):
    heads = gain.shape[0]
    ranks, cut = half.shape
    width = act.shape[1]
    each, quarter = ranks // 2, ranks // 8
    c, hi = place[0], place[2]

    @pl.when(c == 0)
    def _():
        maps[:, 0:cut] = half[...]
        maps[:, cut:] = other[...]

    @pl.when(c != 0)
    def _():
        maps[:, 0:cut] = other[...]
        maps[:, cut:] = half[...]

    def lanes(tile, count=1):
        return pl.ds(pl.multiple_of(tile * HD, HD), count * HD)

    r, k = onto((ranks, ranks), 0), onto((ranks, ranks), 1)
    loc = r % each
    order = (k == 4 * (loc // 2) + 2 * ((r // each) ^ hi) + loc % 2).astype(F32).astype(BF16)
    up = nn(order, nt(maps[:, 0:width], act[...]).astype(BF16)).astype(BF16)
    back = nn(order, nt(maps[:, width:], delta[...]).astype(BF16)).astype(BF16)
    r, k = onto((8 * REM, ranks), 0), onto((8 * REM, ranks), 1)
    at = (r // REM % 2) * each + (r // (2 * REM)) * quarter + r % REM
    pick = ((k == at) & (r % REM < quarter)).astype(F32).astype(BF16)
    rems = nn(pick, back).astype(BF16)
    count = jnp.sum(valid[...].astype(F32))
    row = onto((REM, HD), 0)

    def four(t, _):
        ups = nn(up, delta[:, lanes(4 * t, 4)])
        downs = nn(back, act[:, lanes(4 * t, 4)])
        rests = nn(rems, act[:, lanes(heads + t)])
        for p in range(2):
            i = 2 * t + p
            for x in range(2):
                pieces = []
                for q in (2 * p, 2 * p + 1):
                    cols, rows = slice(q * HD, (q + 1) * HD), slice(x * each, (x + 1) * each)
                    g = jnp.sum(gain[4 * t + q], axis=0, keepdims=True)
                    first = (2 * q + x) * REM
                    rest = rests[first : first + REM]
                    rest = jnp.where(row == quarter, g, jnp.where(row == quarter + 1, count, rest))
                    pieces.append((ups[rows, cols], downs[rows, cols], rest))
                for j, (top, size) in enumerate(((0, each), (each, each), (2 * each, REM))):
                    even, odd = pieces[0][j], pieces[1][j]
                    at = x * (heads // 2) + i
                    mine[at, top : top + size, :] = jnp.where(c == 0, even, odd)
                    theirs[at, top : top + size, :] = jnp.where(c == 0, odd, even).astype(theirs.dtype)
        return 0

    lax.fori_loop(0, heads // 4, four, 0)


def spread_kernel(place, blocks, out, total, ranks, length):
    peers, rows, _ = blocks.shape
    acc = blocks[0].astype(F32)
    for i in range(1, peers):
        acc = acc + blocks[i].astype(F32)
    total[...] = jnp.zeros_like(total)
    total[0:rows, :] = acc
    q = place[1]
    quarter = ranks // 4
    shape = (8 * length, total.shape[0])
    r, k = onto(shape, 0), onto(shape, 1)
    j = r % 8
    at = 2 * (r // 8) + j % 2
    want = jnp.where(j < 2, at, at + ranks)
    rem = jnp.where(at // quarter == q, 2 * ranks + at % quarter, -1)
    want = jnp.where(j < 4, want, rem)
    want = jnp.where(j < 6, want, 2 * ranks + quarter + j - 6)
    pick = (k == want).astype(F32)
    out[...] = lax.dot_general(
        pick, total[...], (((1,), (0,)), ((), ())), precision=lax.Precision.HIGHEST, preferred_element_type=F32
    )


def finish_kernel(parts, down, up, gain, tokens):
    heads = parts.shape[0]
    factor = tokens / parts[0, 7:8, 0:1]
    for s in range(heads):
        b = parts[s] * factor
        up[:, s * HD : (s + 1) * HD] = b[0:2]
        down[:, s * HD : (s + 1) * HD] = b[2:4]
        gain[:, s * HD : (s + 1) * HD] = b[6:7]
    for t in range(heads // 4):
        b = parts[4 * t] + parts[4 * t + 1] + parts[4 * t + 2] + parts[4 * t + 3]
        down[:, (heads + t) * HD : (heads + t + 1) * HD] = b[4:6] * factor


VMEM = pl.BlockSpec(memory_space=pltpu.VMEM)
SMEM = pl.BlockSpec(memory_space=pltpu.SMEM)


def within(mib):
    return pltpu.CompilerParams(vmem_limit_bytes=mib * 2**20)


def gather_ranks(adapter_lowering, adapter_raising, dp, seq, member):
    own = jnp.concatenate([adapter_lowering, adapter_raising], axis=2)
    cut = own.shape[2] // 2
    own = jnp.where(member % 2 == 0, own[:, :, :cut], own[:, :, cut:])
    near = lax.ppermute(own, "dp", [(d, d ^ 1) for d in range(dp)])
    pair = jnp.concatenate([own, near], axis=0)
    along_z = [list(range(hi, dp, 2)) for hi in range(2)]
    half = lax.all_gather(pair, "dp", axis=0, tiled=True, axis_index_groups=along_z)
    half = half.reshape(dp * own.shape[1], cut)
    other = lax.ppermute(half, "seq", [(s, s ^ 1) for s in range(seq)])
    return half, other


def shards(projections, rotated_query_gradient, gains, adapter_lowering, adapter_raising, activations, positions, valid):
    dp, seq = lax.axis_size("dp"), lax.axis_size("seq")
    proj, act = projections[0, 0], activations[0]
    tokens, features = proj.shape
    ranks = dp * adapter_lowering.shape[1]
    member = lax.axis_index("seq")
    tg = rotated_query_gradient.reshape(seq, tokens, HD)
    tg = lax.all_to_all(tg, "seq", 0, 0, tiled=True)
    half, other = gather_ranks(adapter_lowering, adapter_raising, dp, seq, member)
    cosine, sine = rope_tables(positions[:, 0], valid[0])
    rows = ranks + REM
    place = jnp.stack([member % 2, member % 4, lax.axis_index("dp") % 2]).astype(jnp.int32)
    delta, gain = pl.pallas_call(
        delta_kernel,
        out_shape=(
            jax.ShapeDtypeStruct((tokens, features), BF16),
            jax.ShapeDtypeStruct((seq, 8, HD), F32),
        ),
        in_specs=[VMEM] * 5,
        out_specs=(VMEM, VMEM),
        compiler_params=within(6),
        scratch_shapes=[pltpu.VMEM((8, features), F32)],
    )(tg, proj, cosine, sine, gains)
    mine, theirs = pl.pallas_call(
        sums_kernel,
        out_shape=(
            jax.ShapeDtypeStruct((seq, rows, HD), F32),
            jax.ShapeDtypeStruct((seq, rows, HD), BF16),
        ),
        in_specs=[SMEM] + [VMEM] * 6,
        out_specs=(VMEM, VMEM),
        compiler_params=within(8),
        scratch_shapes=[pltpu.VMEM((ranks, act.shape[1] + features), BF16)],
    )(place, act, half, other, delta, gain, valid)
    partner = lax.ppermute(theirs, "seq", [(s, s ^ 1) for s in range(seq)])
    both = (mine + partner.astype(F32)).astype(BF16)
    length = dp // 2
    planes = [
        [(2 * z + x) * seq + 2 * i + c for x in range(2) for i in range(seq // 2)]
        for z in range(length)
        for c in range(2)
    ]
    blocks = lax.all_to_all(both, ("dp", "seq"), 0, 0, tiled=True, axis_index_groups=planes)
    rank_rows = pl.pallas_call(
        lambda *refs: spread_kernel(*refs, ranks=ranks // 2, length=length),
        out_shape=jax.ShapeDtypeStruct((8 * length, HD), F32),
        in_specs=[SMEM, VMEM],
        out_specs=VMEM,
        compiler_params=within(4),
        scratch_shapes=[pltpu.VMEM((128, HD), F32)],
    )(place, blocks)
    along_z = [list(range(hi, dp, 2)) for hi in range(2)]
    shares = lax.all_to_all(rank_rows.reshape(length, 8, HD), "dp", 0, 0, tiled=True, axis_index_groups=along_z)
    share = jnp.sum(shares, axis=0)
    parts = lax.all_to_all(jnp.broadcast_to(share, (seq, 8, HD)), "seq", 0, 0, tiled=True)
    down, up, gain = pl.pallas_call(
        lambda *refs: finish_kernel(*refs, tokens=float(dp * seq * tokens)),
        out_shape=(
            jax.ShapeDtypeStruct((2, act.shape[1]), F32),
            jax.ShapeDtypeStruct((2, features), F32),
            jax.ShapeDtypeStruct((1, features), F32),
        ),
        in_specs=[VMEM],
        out_specs=(VMEM, VMEM, VMEM),
        compiler_params=within(4),
    )(parts)
    return down[None], up[None], gain


def solution(mesh):
    in_specs = (
        P(None, "dp", "seq", None),
        P(None, "dp", None, "seq"),
        P(),
        P(None, "dp", None),
        P(None, "dp", None),
        P("dp", "seq", None),
        P(None, "dp", "seq"),
        P("dp", "seq"),
    )
    out_specs = (P(None, "dp", None), P(None, "dp", None), P())
    return jax.shard_map(shards, mesh=mesh, in_specs=in_specs, out_specs=out_specs, check_vma=False)
```

```python
import jax
import jax.numpy as jnp
import numpy as np
from jax import lax
from jax.experimental import pallas as pl
from jax.experimental.pallas import tpu as pltpu
from jax.sharding import PartitionSpec as P


HD = 128
EPSILON = 1e-06
F32 = jnp.float32
BF16 = jnp.bfloat16

REM = 8


def onto(shape, dim):
    return lax.broadcasted_iota(jnp.int32, shape, dim)


def nt(a, b):
    return lax.dot_general(a, b, (((1,), (1,)), ((), ())), preferred_element_type=F32)


def nn(a, b):
    return lax.dot_general(a, b, (((1,), (0,)), ((), ())), preferred_element_type=F32)


def rope_tables(positions, valid):
    one_sixth = HD // 6
    counts = (HD // 2 - 2 * one_sixth, one_sixth, one_sixth)
    group = np.repeat(np.concatenate([np.full(n, k) for k, n in enumerate(counts)]), 2)
    powers = np.concatenate([-np.arange(n) / n for n in counts])
    frequency = np.repeat((10000.0**powers).astype(np.float32), 2)
    sign = np.where(np.arange(HD) % 2 == 0, 1.0, -1.0).astype(np.float32)
    at = positions.astype(F32)
    index = jnp.where(group == 0, at[0][:, None], jnp.where(group == 1, at[1][:, None], at[2][:, None]))
    angles = index * frequency
    keep = valid.astype(F32)[:, None]
    return jnp.cos(angles) * keep, jnp.sin(angles) * (keep * sign)


def mean_of(parts, features):
    mean = jnp.sum((parts[0] + parts[1]) + (parts[2] + parts[3]), axis=1, keepdims=True) / features
    return jnp.broadcast_to(mean, (8, HD))


def inverse_kernel(proj, cosine, sine, cos, sin, square):
    tokens, features = proj.shape

    def eight(k, _):
        rows = pl.ds(pl.multiple_of(8 * k, 8), 8)
        acc = [jnp.zeros((8, HD), F32)] * 4
        for h in range(features // HD):
            p = proj[rows, h * HD : (h + 1) * HD].astype(F32)
            acc[h % 4] = acc[h % 4] + p * p
        inverse = lax.rsqrt(mean_of(acc, features) + EPSILON)
        cos[rows, :] = cosine[rows, :] * inverse
        sin[rows, :] = sine[rows, :] * inverse
        square[rows, :] = inverse * inverse
        return 0

    lax.fori_loop(0, tokens // 8, eight, 0, unroll=4)


def delta_kernel(tg, proj, cos, sin, square, gains, delta, gain, gains8):
    heads, tokens, _ = tg.shape
    features = heads * HD
    even = onto((8, HD), 1) % 2 == 0
    gain[...] = jnp.zeros_like(gain)
    gains8[...] = jnp.broadcast_to(gains[...], gains8.shape)
    group = 4

    def some(k, _):
        rows = [pl.ds(pl.multiple_of(8 * (group * k + b), 8), 8) for b in range(group)]
        ps = [[proj[r, h * HD : (h + 1) * HD].astype(F32) for h in range(heads)] for r in rows]
        turns = [(cos[r, :], sin[r, :]) for r in rows]
        ws = [[None] * heads for _ in rows]
        acc = [[jnp.zeros((8, HD), F32)] * 4 for _ in rows]
        for h in range(heads):
            gh = gains8[:, h * HD : (h + 1) * HD]
            total = gain[h]
            for b, r in enumerate(rows):
                g = tg[h, r, :].astype(F32)
                turned = jnp.where(even, pltpu.roll(g, HD - 1, 1), pltpu.roll(g, 1, 1))
                u = turns[b][0] * g + turns[b][1] * turned
                p = ps[b][h]
                total = total + u * p
                ws[b][h] = u * gh
                acc[b][h % 4] = acc[b][h % 4] + ws[b][h] * p
            gain[h] = total
        for b, r in enumerate(rows):
            mean = mean_of(acc[b], features) * square[r, :]
            for h in range(heads):
                delta[r, h * HD : (h + 1) * HD] = (ws[b][h] - ps[b][h] * mean).astype(BF16)
        return 0

    lax.fori_loop(0, tokens // (8 * group), some, 0)


def sums_kernel(place, act, half, other, delta, gain, valid, mine, theirs, maps):
    heads = gain.shape[0]
    ranks, cut = half.shape
    width = act.shape[1]
    each, quarter = ranks // 2, ranks // 8
    c, hi = place[0], place[2]

    @pl.when(c == 0)
    def _():
        maps[:, 0:cut] = half[...]
        maps[:, cut:] = other[...]

    @pl.when(c != 0)
    def _():
        maps[:, 0:cut] = other[...]
        maps[:, cut:] = half[...]

    def lanes(tile, count=1):
        return pl.ds(pl.multiple_of(tile * HD, HD), count * HD)

    r, k = onto((ranks, ranks), 0), onto((ranks, ranks), 1)
    loc = r % each
    order = (k == 4 * (loc // 2) + 2 * ((r // each) ^ hi) + loc % 2).astype(F32).astype(BF16)
    up = nt(maps[:, 0:width], act[...]).astype(BF16)
    back = nt(maps[:, width:], delta[...]).astype(BF16)
    up = nn(order, up).astype(BF16)
    back = nn(order, back).astype(BF16)
    r, k = onto((8 * REM, ranks), 0), onto((8 * REM, ranks), 1)
    at = (r // REM % 2) * each + (r // (2 * REM)) * quarter + r % REM
    pick = ((k == at) & (r % REM < quarter)).astype(F32).astype(BF16)
    rems = nn(pick, back).astype(BF16)
    count = jnp.sum(valid[...].astype(F32))
    row = onto((REM, HD), 0)

    def four(t, _):
        ups = nn(up, delta[:, lanes(4 * t, 4)])
        downs = nn(back, act[:, lanes(4 * t, 4)])
        rests = nn(rems, act[:, lanes(heads + t)])
        for p in range(2):
            i = 2 * t + p
            for x in range(2):
                pieces = []
                for q in (2 * p, 2 * p + 1):
                    cols, rows = slice(q * HD, (q + 1) * HD), slice(x * each, (x + 1) * each)
                    g = jnp.sum(gain[4 * t + q], axis=0, keepdims=True)
                    first = (2 * q + x) * REM
                    rest = rests[first : first + REM]
                    rest = jnp.where(row == quarter, g, jnp.where(row == quarter + 1, count, rest))
                    pieces.append((ups[rows, cols], downs[rows, cols], rest))
                for j, (top, size) in enumerate(((0, each), (each, each), (2 * each, REM))):
                    even, odd = pieces[0][j], pieces[1][j]
                    at = x * (heads // 2) + i
                    mine[at, top : top + size, :] = jnp.where(c == 0, even, odd)
                    theirs[at, top : top + size, :] = jnp.where(c == 0, odd, even).astype(theirs.dtype)
        return 0

    lax.fori_loop(0, heads // 4, four, 0, unroll=4)


def spread_kernel(place, blocks, out, total, ranks, length):
    peers, rows, _ = blocks.shape
    acc = blocks[0].astype(F32)
    for i in range(1, peers):
        acc = acc + blocks[i].astype(F32)
    total[...] = jnp.zeros_like(total)
    total[0:rows, :] = acc
    q = place[1]
    quarter = ranks // 4
    shape = (8 * length, total.shape[0])
    r, k = onto(shape, 0), onto(shape, 1)
    j = r % 8
    at = 2 * (r // 8) + j % 2
    want = jnp.where(j < 2, at, at + ranks)
    rem = jnp.where(at // quarter == q, 2 * ranks + at % quarter, -1)
    want = jnp.where(j < 4, want, rem)
    want = jnp.where(j < 6, want, 2 * ranks + quarter + j - 6)
    pick = (k == want).astype(F32)
    out[...] = lax.dot_general(
        pick, total[...], (((1,), (0,)), ((), ())), precision=lax.Precision.HIGHEST, preferred_element_type=F32
    )


def finish_kernel(parts, down, up, gain, tokens):
    heads = parts.shape[0]
    factor = tokens / parts[0, 7:8, 0:1]
    for s in range(heads):
        b = parts[s] * factor
        up[:, s * HD : (s + 1) * HD] = b[0:2]
        down[:, s * HD : (s + 1) * HD] = b[2:4]
        gain[:, s * HD : (s + 1) * HD] = b[6:7]
    for t in range(heads // 4):
        b = parts[4 * t] + parts[4 * t + 1] + parts[4 * t + 2] + parts[4 * t + 3]
        down[:, (heads + t) * HD : (heads + t + 1) * HD] = b[4:6] * factor


VMEM = pl.BlockSpec(memory_space=pltpu.VMEM)
SMEM = pl.BlockSpec(memory_space=pltpu.SMEM)


def within(mib):
    return pltpu.CompilerParams(vmem_limit_bytes=mib * 2**20)


def gather_ranks(adapter_lowering, adapter_raising, dp, seq, member, small):
    own = jnp.concatenate([adapter_lowering, adapter_raising], axis=2)
    cut = own.shape[2] // 2
    own = jnp.where(member % 2 == 0, own[:, :, :cut], own[:, :, cut:])
    near = lax.ppermute(own, "dp", [(d, d ^ 1) for d in range(dp)])
    pair = jnp.concatenate([own, near], axis=0)
    pair, small = lax.optimization_barrier((pair, small))
    along_z = [list(range(hi, dp, 2)) for hi in range(2)]
    half = lax.all_gather(pair, "dp", axis=0, tiled=True, axis_index_groups=along_z)
    half = half.reshape(dp * own.shape[1], cut)
    other = lax.ppermute(half, "seq", [(s, s ^ 1) for s in range(seq)])
    return half, other, small


def shards(projections, rotated_query_gradient, gains, adapter_lowering, adapter_raising, activations, positions, valid):
    dp, seq = lax.axis_size("dp"), lax.axis_size("seq")
    proj, act = projections[0, 0], activations[0]
    tokens, features = proj.shape
    ranks = dp * adapter_lowering.shape[1]
    member = lax.axis_index("seq")
    tg = rotated_query_gradient.reshape(seq, tokens, HD)
    tg = lax.all_to_all(tg, "seq", 0, 0, tiled=True)
    tables = pl.pallas_call(
        inverse_kernel,
        out_shape=(jax.ShapeDtypeStruct((tokens, HD), F32),) * 3,
        in_specs=[VMEM] * 3,
        out_specs=(VMEM,) * 3,
        compiler_params=within(3),
    )(proj, *rope_tables(positions[:, 0], valid[0]))
    half, other, tables = gather_ranks(adapter_lowering, adapter_raising, dp, seq, member, tables)
    rows = ranks + REM
    place = jnp.stack([member % 2, member % 4, lax.axis_index("dp") % 2]).astype(jnp.int32)
    delta, gain = pl.pallas_call(
        delta_kernel,
        out_shape=(
            jax.ShapeDtypeStruct((tokens, features), BF16),
            jax.ShapeDtypeStruct((seq, 8, HD), F32),
        ),
        in_specs=[VMEM] * 6,
        out_specs=(VMEM, VMEM),
        compiler_params=within(6),
        scratch_shapes=[pltpu.VMEM((8, features), F32)],
    )(tg, proj, *tables, gains)
    mine, theirs = pl.pallas_call(
        sums_kernel,
        out_shape=(
            jax.ShapeDtypeStruct((seq, rows, HD), F32),
            jax.ShapeDtypeStruct((seq, rows, HD), BF16),
        ),
        in_specs=[SMEM] + [VMEM] * 6,
        out_specs=(VMEM, VMEM),
        compiler_params=within(8),
        scratch_shapes=[pltpu.VMEM((ranks, act.shape[1] + features), BF16)],
    )(place, act, half, other, delta, gain, valid)
    partner = lax.ppermute(theirs, "seq", [(s, s ^ 1) for s in range(seq)])
    both = (mine + partner.astype(F32)).astype(BF16)
    length = dp // 2
    planes = [
        [(2 * z + x) * seq + 2 * i + c for x in range(2) for i in range(seq // 2)]
        for z in range(length)
        for c in range(2)
    ]
    blocks = lax.all_to_all(both, ("dp", "seq"), 0, 0, tiled=True, axis_index_groups=planes)
    rank_rows = pl.pallas_call(
        lambda *refs: spread_kernel(*refs, ranks=ranks // 2, length=length),
        out_shape=jax.ShapeDtypeStruct((8 * length, HD), F32),
        in_specs=[SMEM, VMEM],
        out_specs=VMEM,
        compiler_params=within(4),
        scratch_shapes=[pltpu.VMEM((128, HD), F32)],
    )(place, blocks)
    along_z = [list(range(hi, dp, 2)) for hi in range(2)]
    shares = lax.all_to_all(rank_rows.reshape(length, 8, HD), "dp", 0, 0, tiled=True, axis_index_groups=along_z)
    share = jnp.sum(shares, axis=0)
    parts = lax.all_to_all(jnp.broadcast_to(share, (seq, 8, HD)), "seq", 0, 0, tiled=True)
    down, up, gain = pl.pallas_call(
        lambda *refs: finish_kernel(*refs, tokens=float(dp * seq * tokens)),
        out_shape=(
            jax.ShapeDtypeStruct((2, act.shape[1]), F32),
            jax.ShapeDtypeStruct((2, features), F32),
            jax.ShapeDtypeStruct((1, features), F32),
        ),
        in_specs=[VMEM],
        out_specs=(VMEM, VMEM, VMEM),
        compiler_params=within(4),
    )(parts)
    return down[None], up[None], gain


def solution(mesh):
    in_specs = (
        P(None, "dp", "seq", None),
        P(None, "dp", None, "seq"),
        P(),
        P(None, "dp", None),
        P(None, "dp", None),
        P("dp", "seq", None),
        P(None, "dp", "seq"),
        P("dp", "seq"),
    )
    out_specs = (P(None, "dp", None), P(None, "dp", None), P())
    return jax.shard_map(shards, mesh=mesh, in_specs=in_specs, out_specs=out_specs, check_vma=False)
```

```python
import jax
import jax.numpy as jnp
import numpy as np
from jax import lax
from jax.experimental import pallas as pl
from jax.experimental.pallas import tpu as pltpu
from jax.sharding import PartitionSpec as P


HD = 128
EPSILON = 1e-06
F32 = jnp.float32
BF16 = jnp.bfloat16

REM = 8


def onto(shape, dim):
    return lax.broadcasted_iota(jnp.int32, shape, dim)


def nt(a, b):
    return lax.dot_general(a, b, (((1,), (1,)), ((), ())), preferred_element_type=F32)


def nn(a, b):
    return lax.dot_general(a, b, (((1,), (0,)), ((), ())), preferred_element_type=F32)


def rope_tables(positions, valid):
    one_sixth = HD // 6
    counts = (HD // 2 - 2 * one_sixth, one_sixth, one_sixth)
    group = np.repeat(np.concatenate([np.full(n, k) for k, n in enumerate(counts)]), 2)
    powers = np.concatenate([-np.arange(n) / n for n in counts])
    frequency = np.repeat((10000.0**powers).astype(np.float32), 2)
    sign = np.where(np.arange(HD) % 2 == 0, 1.0, -1.0).astype(np.float32)
    at = positions.astype(F32)
    index = jnp.where(group == 0, at[0][:, None], jnp.where(group == 1, at[1][:, None], at[2][:, None]))
    angles = index * frequency
    keep = valid.astype(F32)[:, None]
    return jnp.cos(angles) * keep, jnp.sin(angles) * (keep * sign)


def mean_of(parts, features):
    mean = jnp.sum((parts[0] + parts[1]) + (parts[2] + parts[3]), axis=1, keepdims=True) / features
    return jnp.broadcast_to(mean, (8, HD))


def inverse_kernel(proj, cosine, sine, cos, sin, square):
    tokens, features = proj.shape

    def eight(k, _):
        rows = pl.ds(pl.multiple_of(8 * k, 8), 8)
        acc = [jnp.zeros((8, HD), F32)] * 4
        for h in range(features // HD):
            p = proj[rows, h * HD : (h + 1) * HD].astype(F32)
            acc[h % 4] = acc[h % 4] + p * p
        inverse = lax.rsqrt(mean_of(acc, features) + EPSILON)
        cos[rows, :] = cosine[rows, :] * inverse
        sin[rows, :] = sine[rows, :] * inverse
        square[rows, :] = inverse * inverse
        return 0

    lax.fori_loop(0, tokens // 8, eight, 0, unroll=4)


def delta_kernel(tg, proj, cos, sin, square, gains, delta, gain, gains8):
    heads, tokens, _ = tg.shape
    features = heads * HD
    even = onto((8, HD), 1) % 2 == 0
    gain[...] = jnp.zeros_like(gain)
    gains8[...] = jnp.broadcast_to(gains[...], gains8.shape)
    group = 4

    def some(k, _):
        rows = [pl.ds(pl.multiple_of(8 * (group * k + b), 8), 8) for b in range(group)]
        ps = [[proj[r, h * HD : (h + 1) * HD].astype(F32) for h in range(heads)] for r in rows]
        turns = [(cos[r, :], sin[r, :]) for r in rows]
        ws = [[None] * heads for _ in rows]
        acc = [[jnp.zeros((8, HD), F32)] * 4 for _ in rows]
        for h in range(heads):
            gh = gains8[:, h * HD : (h + 1) * HD]
            total = gain[h]
            for b, r in enumerate(rows):
                g = tg[h, r, :].astype(F32)
                turned = jnp.where(even, pltpu.roll(g, HD - 1, 1), pltpu.roll(g, 1, 1))
                u = turns[b][0] * g + turns[b][1] * turned
                p = ps[b][h]
                total = total + u * p
                ws[b][h] = u * gh
                acc[b][h % 4] = acc[b][h % 4] + ws[b][h] * p
            gain[h] = total
        for b, r in enumerate(rows):
            mean = mean_of(acc[b], features) * square[r, :]
            for h in range(heads):
                delta[r, h * HD : (h + 1) * HD] = (ws[b][h] - ps[b][h] * mean).astype(BF16)
        return 0

    lax.fori_loop(0, tokens // (8 * group), some, 0)


def sums_kernel(act, half, other, delta, gain, valid, mine, theirs, maps):
    heads = gain.shape[0]
    ranks, cut = half.shape
    width = act.shape[1]
    each, quarter = ranks // 2, ranks // 8
    c, hi = lax.axis_index("seq") % 2, lax.axis_index("dp") % 2

    @pl.when(c == 0)
    def _():
        maps[:, 0:cut] = half[...]
        maps[:, cut:] = other[...]

    @pl.when(c != 0)
    def _():
        maps[:, 0:cut] = other[...]
        maps[:, cut:] = half[...]

    def lanes(tile, count=1):
        return pl.ds(pl.multiple_of(tile * HD, HD), count * HD)

    r, k = onto((ranks, ranks), 0), onto((ranks, ranks), 1)
    far = (r >= each).astype(jnp.int32)
    loc = r - each * far
    order = (k == 2 * loc - (loc & 1) + 2 * (far ^ hi)).astype(F32).astype(BF16)
    up = nt(maps[:, 0:width], act[...]).astype(BF16)
    back = nt(maps[:, width:], delta[...]).astype(BF16)
    up = nn(order, up).astype(BF16)
    back = nn(order, back).astype(BF16)
    r, k = onto((8 * REM, ranks), 0), onto((8 * REM, ranks), 1)
    at = ((r >> 3) & 1) * each + (r >> 4) * quarter + (r & 7)
    pick = ((k == at) & ((r & 7) < quarter)).astype(F32).astype(BF16)
    rems = nn(pick, back).astype(BF16)
    count = jnp.sum(valid[...].astype(F32))
    row = onto((REM, HD), 0)

    def four(t, _):
        ups = nn(up, delta[:, lanes(4 * t, 4)])
        downs = nn(back, act[:, lanes(4 * t, 4)])
        rests = nn(rems, act[:, lanes(heads + t)])
        for p in range(2):
            i = 2 * t + p
            for x in range(2):
                pieces = []
                for q in (2 * p, 2 * p + 1):
                    cols, rows = slice(q * HD, (q + 1) * HD), slice(x * each, (x + 1) * each)
                    g = jnp.sum(gain[4 * t + q], axis=0, keepdims=True)
                    first = (2 * q + x) * REM
                    rest = rests[first : first + REM]
                    rest = jnp.where(row == quarter, g, jnp.where(row == quarter + 1, count, rest))
                    pieces.append((ups[rows, cols], downs[rows, cols], rest))
                for j, (top, size) in enumerate(((0, each), (each, each), (2 * each, REM))):
                    even, odd = pieces[0][j], pieces[1][j]
                    at = x * (heads // 2) + i
                    mine[at, top : top + size, :] = jnp.where(c == 0, even, odd)
                    theirs[at, top : top + size, :] = jnp.where(c == 0, odd, even).astype(theirs.dtype)
        return 0

    lax.fori_loop(0, heads // 4, four, 0, unroll=4)


def spread_kernel(blocks, out, total, ranks, length):
    peers, rows, _ = blocks.shape
    acc = blocks[0].astype(F32)
    for i in range(1, peers):
        acc = acc + blocks[i].astype(F32)
    total[...] = jnp.zeros_like(total)
    total[0:rows, :] = acc
    q = lax.axis_index("seq") % 4
    quarter = ranks // 4
    shape = (8 * length, total.shape[0])
    r, k = onto(shape, 0), onto(shape, 1)
    j = r & 7
    at = 2 * (r >> 3) + (j & 1)
    want = jnp.where(j < 2, at, at + ranks)
    rem = at - quarter * q
    rem = jnp.where((rem >= 0) & (rem < quarter), 2 * ranks + rem, -1)
    want = jnp.where(j < 4, want, rem)
    want = jnp.where(j < 6, want, 2 * ranks + quarter + j - 6)
    pick = (k == want).astype(F32)
    out[...] = lax.dot_general(
        pick, total[...], (((1,), (0,)), ((), ())), precision=lax.Precision.HIGHEST, preferred_element_type=F32
    )


def finish_kernel(parts, down, up, gain, tokens):
    heads = parts.shape[0]
    factor = tokens / parts[0, 7:8, 0:1]
    for s in range(heads):
        b = parts[s] * factor
        up[:, s * HD : (s + 1) * HD] = b[0:2]
        down[:, s * HD : (s + 1) * HD] = b[2:4]
        gain[:, s * HD : (s + 1) * HD] = b[6:7]
    for t in range(heads // 4):
        b = parts[4 * t] + parts[4 * t + 1] + parts[4 * t + 2] + parts[4 * t + 3]
        down[:, (heads + t) * HD : (heads + t + 1) * HD] = b[4:6] * factor


VMEM = pl.BlockSpec(memory_space=pltpu.VMEM)


def within(mib):
    return pltpu.CompilerParams(vmem_limit_bytes=mib * 2**20)


def gather_ranks(adapter_lowering, adapter_raising, dp, seq, member, small):
    own = jnp.concatenate([adapter_lowering, adapter_raising], axis=2)
    cut = own.shape[2] // 2
    own = jnp.where(member % 2 == 0, own[:, :, :cut], own[:, :, cut:])
    near = lax.ppermute(own, "dp", [(d, d ^ 1) for d in range(dp)])
    pair = jnp.concatenate([own, near], axis=0)
    pair, small = lax.optimization_barrier((pair, small))
    along_z = [list(range(hi, dp, 2)) for hi in range(2)]
    half = lax.all_gather(pair, "dp", axis=0, tiled=True, axis_index_groups=along_z)
    half = half.reshape(dp * own.shape[1], cut)
    other = lax.ppermute(half, "seq", [(s, s ^ 1) for s in range(seq)])
    return half, other, small


def shards(projections, rotated_query_gradient, gains, adapter_lowering, adapter_raising, activations, positions, valid):
    dp, seq = lax.axis_size("dp"), lax.axis_size("seq")
    proj, act = projections[0, 0], activations[0]
    tokens, features = proj.shape
    ranks = dp * adapter_lowering.shape[1]
    member = lax.axis_index("seq")
    tg = rotated_query_gradient.reshape(seq, tokens, HD)
    tg = lax.all_to_all(tg, "seq", 0, 0, tiled=True)
    tables = pl.pallas_call(
        inverse_kernel,
        out_shape=(jax.ShapeDtypeStruct((tokens, HD), F32),) * 3,
        in_specs=[VMEM] * 3,
        out_specs=(VMEM,) * 3,
        compiler_params=within(3),
    )(proj, *rope_tables(positions[:, 0], valid[0]))
    half, other, tables = gather_ranks(adapter_lowering, adapter_raising, dp, seq, member, tables)
    rows = ranks + REM
    delta, gain = pl.pallas_call(
        delta_kernel,
        out_shape=(
            jax.ShapeDtypeStruct((tokens, features), BF16),
            jax.ShapeDtypeStruct((seq, 8, HD), F32),
        ),
        in_specs=[VMEM] * 6,
        out_specs=(VMEM, VMEM),
        compiler_params=within(6),
        scratch_shapes=[pltpu.VMEM((8, features), F32)],
    )(tg, proj, *tables, gains)
    mine, theirs = pl.pallas_call(
        sums_kernel,
        out_shape=(
            jax.ShapeDtypeStruct((seq, rows, HD), F32),
            jax.ShapeDtypeStruct((seq, rows, HD), BF16),
        ),
        in_specs=[VMEM] * 6,
        out_specs=(VMEM, VMEM),
        compiler_params=within(8),
        scratch_shapes=[pltpu.VMEM((ranks, act.shape[1] + features), BF16)],
    )(act, half, other, delta, gain, valid)
    partner = lax.ppermute(theirs, "seq", [(s, s ^ 1) for s in range(seq)])
    both = (mine + partner.astype(F32)).astype(BF16)
    length = dp // 2
    planes = [
        [(2 * z + x) * seq + 2 * i + c for x in range(2) for i in range(seq // 2)]
        for z in range(length)
        for c in range(2)
    ]
    blocks = lax.all_to_all(both, ("dp", "seq"), 0, 0, tiled=True, axis_index_groups=planes)
    rank_rows = pl.pallas_call(
        lambda *refs: spread_kernel(*refs, ranks=ranks // 2, length=length),
        out_shape=jax.ShapeDtypeStruct((8 * length, HD), F32),
        in_specs=[VMEM],
        out_specs=VMEM,
        compiler_params=within(4),
        scratch_shapes=[pltpu.VMEM((128, HD), F32)],
    )(blocks)
    along_z = [list(range(hi, dp, 2)) for hi in range(2)]
    shares = lax.all_to_all(rank_rows.reshape(length, 8, HD), "dp", 0, 0, tiled=True, axis_index_groups=along_z)
    share = jnp.sum(shares, axis=0)
    parts = lax.all_to_all(jnp.broadcast_to(share, (seq, 8, HD)), "seq", 0, 0, tiled=True)
    down, up, gain = pl.pallas_call(
        lambda *refs: finish_kernel(*refs, tokens=float(dp * seq * tokens)),
        out_shape=(
            jax.ShapeDtypeStruct((2, act.shape[1]), F32),
            jax.ShapeDtypeStruct((2, features), F32),
            jax.ShapeDtypeStruct((1, features), F32),
        ),
        in_specs=[VMEM],
        out_specs=(VMEM, VMEM, VMEM),
        compiler_params=within(4),
    )(parts)
    return down[None], up[None], gain


def solution(mesh):
    in_specs = (
        P(None, "dp", "seq", None),
        P(None, "dp", None, "seq"),
        P(),
        P(None, "dp", None),
        P(None, "dp", None),
        P("dp", "seq", None),
        P(None, "dp", "seq"),
        P("dp", "seq"),
    )
    out_specs = (P(None, "dp", None), P(None, "dp", None), P())
    return jax.shard_map(shards, mesh=mesh, in_specs=in_specs, out_specs=out_specs, check_vma=False)
```

```python
import jax
import jax.numpy as jnp
import numpy as np
from jax import lax
from jax.experimental import pallas as pl
from jax.experimental.pallas import tpu as pltpu
from jax.sharding import PartitionSpec as P


HD = 128
EPSILON = 1e-06
F32 = jnp.float32
BF16 = jnp.bfloat16

REM = 8


def onto(shape, dim):
    return lax.broadcasted_iota(jnp.int32, shape, dim)


def nt(a, b):
    return lax.dot_general(a, b, (((1,), (1,)), ((), ())), preferred_element_type=F32)


def nn(a, b):
    return lax.dot_general(a, b, (((1,), (0,)), ((), ())), preferred_element_type=F32)


def rope_tables(positions, valid):
    one_sixth = HD // 6
    counts = (HD // 2 - 2 * one_sixth, one_sixth, one_sixth)
    group = np.repeat(np.concatenate([np.full(n, k) for k, n in enumerate(counts)]), 2)
    powers = np.concatenate([-np.arange(n) / n for n in counts])
    frequency = np.repeat((10000.0**powers).astype(np.float32), 2)
    sign = np.where(np.arange(HD) % 2 == 0, 1.0, -1.0).astype(np.float32)
    at = positions.astype(F32)
    index = jnp.where(group == 0, at[0][:, None], jnp.where(group == 1, at[1][:, None], at[2][:, None]))
    angles = index * frequency
    keep = valid.astype(F32)[:, None]
    return jnp.cos(angles) * keep, jnp.sin(angles) * (keep * sign)


def mean_of(parts, features):
    mean = jnp.sum((parts[0] + parts[1]) + (parts[2] + parts[3]), axis=1, keepdims=True) / features
    return jnp.broadcast_to(mean, (8, HD))


def inverse_kernel(proj, cosine, sine, cos, sin, square):
    tokens, features = proj.shape

    def eight(k, _):
        rows = pl.ds(pl.multiple_of(8 * k, 8), 8)
        acc = [jnp.zeros((8, HD), F32)] * 4
        for h in range(features // HD):
            p = proj[rows, h * HD : (h + 1) * HD].astype(F32)
            acc[h % 4] = acc[h % 4] + p * p
        inverse = lax.rsqrt(mean_of(acc, features) + EPSILON)
        cos[rows, :] = cosine[rows, :] * inverse
        sin[rows, :] = sine[rows, :] * inverse
        square[rows, :] = inverse * inverse
        return 0

    lax.fori_loop(0, tokens // 8, eight, 0, unroll=4)


def delta_kernel(tg, proj, cos, sin, square, gains, delta, gain, gains8):
    heads, tokens, _ = tg.shape
    features = heads * HD
    even = onto((8, HD), 1) % 2 == 0
    gain[...] = jnp.zeros_like(gain)
    gains8[...] = jnp.broadcast_to(gains[...], gains8.shape)
    group = 4

    def some(k, _):
        rows = [pl.ds(pl.multiple_of(8 * (group * k + b), 8), 8) for b in range(group)]
        ps = [[proj[r, h * HD : (h + 1) * HD].astype(F32) for h in range(heads)] for r in rows]
        turns = [(cos[r, :], sin[r, :]) for r in rows]
        ws = [[None] * heads for _ in rows]
        acc = [[jnp.zeros((8, HD), F32)] * 4 for _ in rows]
        for h in range(heads):
            gh = gains8[:, h * HD : (h + 1) * HD]
            total = gain[h]
            for b, r in enumerate(rows):
                g = tg[h, r, :].astype(F32)
                turned = jnp.where(even, pltpu.roll(g, HD - 1, 1), pltpu.roll(g, 1, 1))
                u = turns[b][0] * g + turns[b][1] * turned
                p = ps[b][h]
                total = total + u * p
                ws[b][h] = u * gh
                acc[b][h % 4] = acc[b][h % 4] + ws[b][h] * p
            gain[h] = total
        for b, r in enumerate(rows):
            mean = mean_of(acc[b], features) * square[r, :]
            for h in range(heads):
                delta[r, h * HD : (h + 1) * HD] = (ws[b][h] - ps[b][h] * mean).astype(BF16)
        return 0

    lax.fori_loop(0, tokens // (8 * group), some, 0)


def sums_kernel(act, half, other, delta, gain, valid, mine, theirs, maps):
    heads = gain.shape[0]
    ranks, cut = half.shape
    width = act.shape[1]
    each, quarter = ranks // 2, ranks // 8
    c, hi = lax.axis_index("seq") % 2, lax.axis_index("dp") % 2
    part = (lax.axis_index("seq") + lax.axis_index("dp") // 2) % 2

    @pl.when(part == 0)
    def _():
        maps[:, 0:cut] = half[...]
        maps[:, cut:] = other[...]

    @pl.when(part != 0)
    def _():
        maps[:, 0:cut] = other[...]
        maps[:, cut:] = half[...]

    def lanes(tile, count=1):
        return pl.ds(pl.multiple_of(tile * HD, HD), count * HD)

    r, k = onto((ranks, ranks), 0), onto((ranks, ranks), 1)
    far = (r >= each).astype(jnp.int32)
    loc = r - each * far
    order = (k == 2 * loc - (loc & 1) + 2 * (far ^ hi)).astype(F32).astype(BF16)
    up = nt(maps[:, 0:width], act[...]).astype(BF16)
    back = nt(maps[:, width:], delta[...]).astype(BF16)
    up = nn(order, up).astype(BF16)
    back = nn(order, back).astype(BF16)
    r, k = onto((8 * REM, ranks), 0), onto((8 * REM, ranks), 1)
    at = ((r >> 3) & 1) * each + (r >> 4) * quarter + (r & 7)
    pick = ((k == at) & ((r & 7) < quarter)).astype(F32).astype(BF16)
    rems = nn(pick, back).astype(BF16)
    count = jnp.sum(valid[...].astype(F32))
    row = onto((REM, HD), 0)

    def four(t, _):
        ups = nn(up, delta[:, lanes(4 * t, 4)])
        downs = nn(back, act[:, lanes(4 * t, 4)])
        rests = nn(rems, act[:, lanes(heads + t)])
        for p in range(2):
            i = 2 * t + p
            for x in range(2):
                pieces = []
                for q in (2 * p, 2 * p + 1):
                    cols, rows = slice(q * HD, (q + 1) * HD), slice(x * each, (x + 1) * each)
                    g = jnp.sum(gain[4 * t + q], axis=0, keepdims=True)
                    first = (2 * q + x) * REM
                    rest = rests[first : first + REM]
                    rest = jnp.where(row == quarter, g, jnp.where(row == quarter + 1, count, rest))
                    pieces.append((ups[rows, cols], downs[rows, cols], rest))
                for j, (top, size) in enumerate(((0, each), (each, each), (2 * each, REM))):
                    even, odd = pieces[0][j], pieces[1][j]
                    at = x * (heads // 2) + i
                    mine[at, top : top + size, :] = jnp.where(c == 0, even, odd)
                    theirs[at, top : top + size, :] = jnp.where(c == 0, odd, even).astype(theirs.dtype)
        return 0

    lax.fori_loop(0, heads // 4, four, 0, unroll=4)


def spread_kernel(blocks, out, total, ranks, length):
    peers, rows, _ = blocks.shape
    acc = blocks[0].astype(F32)
    for i in range(1, peers):
        acc = acc + blocks[i].astype(F32)
    total[...] = jnp.zeros_like(total)
    total[0:rows, :] = acc
    q = lax.axis_index("seq") % 4
    quarter = ranks // 4
    shape = (8 * length, total.shape[0])
    r, k = onto(shape, 0), onto(shape, 1)
    j = r & 7
    at = 2 * (r >> 3) + (j & 1)
    want = jnp.where(j < 2, at, at + ranks)
    rem = at - quarter * q
    rem = jnp.where((rem >= 0) & (rem < quarter), 2 * ranks + rem, -1)
    want = jnp.where(j < 4, want, rem)
    want = jnp.where(j < 6, want, 2 * ranks + quarter + j - 6)
    pick = (k == want).astype(F32)
    out[...] = lax.dot_general(
        pick, total[...], (((1,), (0,)), ((), ())), precision=lax.Precision.HIGHEST, preferred_element_type=F32
    )


def finish_kernel(parts, down, up, gain, tokens):
    heads = parts.shape[0]
    factor = tokens / parts[0, 7:8, 0:1]
    for s in range(heads):
        b = parts[s] * factor
        up[:, s * HD : (s + 1) * HD] = b[0:2]
        down[:, s * HD : (s + 1) * HD] = b[2:4]
        gain[:, s * HD : (s + 1) * HD] = b[6:7]
    for t in range(heads // 4):
        b = parts[4 * t] + parts[4 * t + 1] + parts[4 * t + 2] + parts[4 * t + 3]
        down[:, (heads + t) * HD : (heads + t + 1) * HD] = b[4:6] * factor


VMEM = pl.BlockSpec(memory_space=pltpu.VMEM)


def within(mib):
    return pltpu.CompilerParams(vmem_limit_bytes=mib * 2**20)


def gather_ranks(adapter_lowering, adapter_raising, dp, seq, member, small):
    own = jnp.concatenate([adapter_lowering, adapter_raising], axis=2)
    cut = own.shape[2] // 2
    part = (member + lax.axis_index("dp") // 2) % 2
    own = jnp.where(part == 0, own[:, :, :cut], own[:, :, cut:])
    near = lax.ppermute(own, "dp", [(d, d ^ 1) for d in range(dp)])
    pair = jnp.concatenate([own, near], axis=0)
    pair, small = lax.optimization_barrier((pair, small))
    rings = [
        [(2 * z + hi) * seq + chip + (first + z) % 2 for z in range(dp // 2)]
        for hi in range(2)
        for chip in range(0, seq, 2)
        for first in range(2)
    ]
    half = lax.all_gather(pair, ("dp", "seq"), axis=0, tiled=True, axis_index_groups=rings)
    half = half.reshape(dp * own.shape[1], cut)
    other = lax.ppermute(half, "seq", [(s, s ^ 1) for s in range(seq)])
    return half, other, small


def shards(projections, rotated_query_gradient, gains, adapter_lowering, adapter_raising, activations, positions, valid):
    dp, seq = lax.axis_size("dp"), lax.axis_size("seq")
    proj, act = projections[0, 0], activations[0]
    tokens, features = proj.shape
    ranks = dp * adapter_lowering.shape[1]
    member = lax.axis_index("seq")
    tg = rotated_query_gradient.reshape(seq, tokens, HD)
    tg = lax.all_to_all(tg, "seq", 0, 0, tiled=True)
    tables = pl.pallas_call(
        inverse_kernel,
        out_shape=(jax.ShapeDtypeStruct((tokens, HD), F32),) * 3,
        in_specs=[VMEM] * 3,
        out_specs=(VMEM,) * 3,
        compiler_params=within(3),
    )(proj, *rope_tables(positions[:, 0], valid[0]))
    half, other, tables = gather_ranks(adapter_lowering, adapter_raising, dp, seq, member, tables)
    rows = ranks + REM
    delta, gain = pl.pallas_call(
        delta_kernel,
        out_shape=(
            jax.ShapeDtypeStruct((tokens, features), BF16),
            jax.ShapeDtypeStruct((seq, 8, HD), F32),
        ),
        in_specs=[VMEM] * 6,
        out_specs=(VMEM, VMEM),
        compiler_params=within(6),
        scratch_shapes=[pltpu.VMEM((8, features), F32)],
    )(tg, proj, *tables, gains)
    mine, theirs = pl.pallas_call(
        sums_kernel,
        out_shape=(
            jax.ShapeDtypeStruct((seq, rows, HD), F32),
            jax.ShapeDtypeStruct((seq, rows, HD), BF16),
        ),
        in_specs=[VMEM] * 6,
        out_specs=(VMEM, VMEM),
        compiler_params=within(8),
        scratch_shapes=[pltpu.VMEM((ranks, act.shape[1] + features), BF16)],
    )(act, half, other, delta, gain, valid)
    partner = lax.ppermute(theirs, "seq", [(s, s ^ 1) for s in range(seq)])
    both = (mine + partner.astype(F32)).astype(BF16)
    length = dp // 2
    planes = [
        [(2 * z + x) * seq + 2 * i + c for x in range(2) for i in range(seq // 2)]
        for z in range(length)
        for c in range(2)
    ]
    blocks = lax.all_to_all(both, ("dp", "seq"), 0, 0, tiled=True, axis_index_groups=planes)
    rank_rows = pl.pallas_call(
        lambda *refs: spread_kernel(*refs, ranks=ranks // 2, length=length),
        out_shape=jax.ShapeDtypeStruct((8 * length, HD), F32),
        in_specs=[VMEM],
        out_specs=VMEM,
        compiler_params=within(4),
        scratch_shapes=[pltpu.VMEM((128, HD), F32)],
    )(blocks)
    along_z = [list(range(hi, dp, 2)) for hi in range(2)]
    shares = lax.all_to_all(rank_rows.reshape(length, 8, HD), "dp", 0, 0, tiled=True, axis_index_groups=along_z)
    share = jnp.sum(shares, axis=0)
    parts = lax.all_to_all(jnp.broadcast_to(share, (seq, 8, HD)), "seq", 0, 0, tiled=True)
    down, up, gain = pl.pallas_call(
        lambda *refs: finish_kernel(*refs, tokens=float(dp * seq * tokens)),
        out_shape=(
            jax.ShapeDtypeStruct((2, act.shape[1]), F32),
            jax.ShapeDtypeStruct((2, features), F32),
            jax.ShapeDtypeStruct((1, features), F32),
        ),
        in_specs=[VMEM],
        out_specs=(VMEM, VMEM, VMEM),
        compiler_params=within(4),
    )(parts)
    return down[None], up[None], gain


def solution(mesh):
    in_specs = (
        P(None, "dp", "seq", None),
        P(None, "dp", None, "seq"),
        P(),
        P(None, "dp", None),
        P(None, "dp", None),
        P("dp", "seq", None),
        P(None, "dp", "seq"),
        P("dp", "seq"),
    )
    out_specs = (P(None, "dp", None), P(None, "dp", None), P())
    return jax.shard_map(shards, mesh=mesh, in_specs=in_specs, out_specs=out_specs, check_vma=False)
```

```python
import jax
import jax.numpy as jnp
import numpy as np
from jax import lax
from jax.experimental import pallas as pl
from jax.experimental.pallas import tpu as pltpu
from jax.sharding import PartitionSpec as P


HD = 128
EPSILON = 1e-06
F32 = jnp.float32
BF16 = jnp.bfloat16

REM = 8


def onto(shape, dim):
    return lax.broadcasted_iota(jnp.int32, shape, dim)


def parity(video, member, dp, seq):
    return (member + 2 * member // seq + 2 * video // dp) % 2


def own_parity():
    return parity(lax.axis_index("dp"), lax.axis_index("seq"), lax.axis_size("dp"), lax.axis_size("seq"))


def nt(a, b):
    return lax.dot_general(a, b, (((1,), (1,)), ((), ())), preferred_element_type=F32)


def nn(a, b):
    return lax.dot_general(a, b, (((1,), (0,)), ((), ())), preferred_element_type=F32)


def rope_tables(positions, valid):
    one_sixth = HD // 6
    counts = (HD // 2 - 2 * one_sixth, one_sixth, one_sixth)
    group = np.repeat(np.concatenate([np.full(n, k) for k, n in enumerate(counts)]), 2)
    powers = np.concatenate([-np.arange(n) / n for n in counts])
    frequency = np.repeat((10000.0**powers).astype(np.float32), 2)
    sign = np.where(np.arange(HD) % 2 == 0, 1.0, -1.0).astype(np.float32)
    at = positions.astype(F32)
    index = jnp.where(group == 0, at[0][:, None], jnp.where(group == 1, at[1][:, None], at[2][:, None]))
    angles = index * frequency
    keep = valid.astype(F32)[:, None]
    return jnp.cos(angles) * keep, jnp.sin(angles) * (keep * sign)


def mean_of(parts, features):
    mean = jnp.sum((parts[0] + parts[1]) + (parts[2] + parts[3]), axis=1, keepdims=True) / features
    return jnp.broadcast_to(mean, (8, HD))


def inverse_kernel(proj, cosine, sine, cos, sin, square):
    tokens, features = proj.shape

    def eight(k, _):
        rows = pl.ds(pl.multiple_of(8 * k, 8), 8)
        acc = [jnp.zeros((8, HD), F32)] * 4
        for h in range(features // HD):
            p = proj[rows, h * HD : (h + 1) * HD].astype(F32)
            acc[h % 4] = acc[h % 4] + p * p
        inverse = lax.rsqrt(mean_of(acc, features) + EPSILON)
        cos[rows, :] = cosine[rows, :] * inverse
        sin[rows, :] = sine[rows, :] * inverse
        square[rows, :] = inverse * inverse
        return 0

    lax.fori_loop(0, tokens // 8, eight, 0, unroll=4)


def delta_kernel(tg, proj, cos, sin, square, gains, delta, gain, gains8):
    heads, tokens, _ = tg.shape
    features = heads * HD
    even = onto((8, HD), 1) % 2 == 0
    gain[...] = jnp.zeros_like(gain)
    gains8[...] = jnp.broadcast_to(gains[...], gains8.shape)
    group = 4

    def some(k, _):
        rows = [pl.ds(pl.multiple_of(8 * (group * k + b), 8), 8) for b in range(group)]
        ps = [[proj[r, h * HD : (h + 1) * HD].astype(F32) for h in range(heads)] for r in rows]
        turns = [(cos[r, :], sin[r, :]) for r in rows]
        ws = [[None] * heads for _ in rows]
        acc = [[jnp.zeros((8, HD), F32)] * 4 for _ in rows]
        for h in range(heads):
            gh = gains8[:, h * HD : (h + 1) * HD]
            total = gain[h]
            for b, r in enumerate(rows):
                g = tg[h, r, :].astype(F32)
                turned = jnp.where(even, pltpu.roll(g, HD - 1, 1), pltpu.roll(g, 1, 1))
                u = turns[b][0] * g + turns[b][1] * turned
                p = ps[b][h]
                total = total + u * p
                ws[b][h] = u * gh
                acc[b][h % 4] = acc[b][h % 4] + ws[b][h] * p
            gain[h] = total
        for b, r in enumerate(rows):
            mean = mean_of(acc[b], features) * square[r, :]
            for h in range(heads):
                delta[r, h * HD : (h + 1) * HD] = (ws[b][h] - ps[b][h] * mean).astype(BF16)
        return 0

    lax.fori_loop(0, tokens // (8 * group), some, 0)


def sums_kernel(act, half, other, delta, gain, valid, mine, theirs, maps):
    heads = gain.shape[0]
    ranks, cut = half.shape
    width = act.shape[1]
    each, quarter = ranks // 2, ranks // 8
    c, hi = own_parity(), lax.axis_index("dp") % 2
    part = (lax.axis_index("seq") + lax.axis_index("dp") // 2) % 2

    @pl.when(part == 0)
    def _():
        maps[:, 0:cut] = half[...]
        maps[:, cut:] = other[...]

    @pl.when(part != 0)
    def _():
        maps[:, 0:cut] = other[...]
        maps[:, cut:] = half[...]

    def lanes(tile, count=1):
        return pl.ds(pl.multiple_of(tile * HD, HD), count * HD)

    r, k = onto((ranks, ranks), 0), onto((ranks, ranks), 1)
    far = (r >= each).astype(jnp.int32)
    loc = r - each * far
    order = (k == 2 * loc - (loc & 1) + 2 * (far ^ hi)).astype(F32).astype(BF16)
    up = nt(maps[:, 0:width], act[...]).astype(BF16)
    back = nt(maps[:, width:], delta[...]).astype(BF16)
    up = nn(order, up).astype(BF16)
    back = nn(order, back).astype(BF16)
    r, k = onto((8 * REM, ranks), 0), onto((8 * REM, ranks), 1)
    at = ((r >> 3) & 1) * each + (r >> 4) * quarter + (r & 7)
    pick = ((k == at) & ((r & 7) < quarter)).astype(F32).astype(BF16)
    rems = nn(pick, back).astype(BF16)
    count = jnp.sum(valid[...].astype(F32))
    row = onto((REM, HD), 0)

    def four(t, _):
        ups = nn(up, delta[:, lanes(4 * t, 4)])
        downs = nn(back, act[:, lanes(4 * t, 4)])
        rests = nn(rems, act[:, lanes(heads + t)])
        for p in range(2):
            i = 2 * t + p
            for x in range(2):
                pieces = []
                for q in (2 * p, 2 * p + 1):
                    cols, rows = slice(q * HD, (q + 1) * HD), slice(x * each, (x + 1) * each)
                    g = jnp.sum(gain[4 * t + q], axis=0, keepdims=True)
                    first = (2 * q + x) * REM
                    rest = rests[first : first + REM]
                    rest = jnp.where(row == quarter, g, jnp.where(row == quarter + 1, count, rest))
                    pieces.append((ups[rows, cols], downs[rows, cols], rest))
                for j, (top, size) in enumerate(((0, each), (each, each), (2 * each, REM))):
                    even, odd = pieces[0][j], pieces[1][j]
                    at = x * (heads // 2) + i
                    mine[at, top : top + size, :] = jnp.where(c == 0, even, odd)
                    theirs[at, top : top + size, :] = jnp.where(c == 0, odd, even).astype(theirs.dtype)
        return 0

    lax.fori_loop(0, heads // 4, four, 0, unroll=4)


def spread_kernel(blocks, out, total, ranks, length):
    peers, rows, _ = blocks.shape
    acc = blocks[0].astype(F32)
    for i in range(1, peers):
        acc = acc + blocks[i].astype(F32)
    total[...] = jnp.zeros_like(total)
    total[0:rows, :] = acc
    q = lax.axis_index("seq") // 2 % 2 * 2 + own_parity()
    quarter = ranks // 4
    shape = (8 * length, total.shape[0])
    r, k = onto(shape, 0), onto(shape, 1)
    j = r & 7
    at = 2 * (r >> 3) + (j & 1)
    want = jnp.where(j < 2, at, at + ranks)
    rem = at - quarter * q
    rem = jnp.where((rem >= 0) & (rem < quarter), 2 * ranks + rem, -1)
    want = jnp.where(j < 4, want, rem)
    want = jnp.where(j < 6, want, 2 * ranks + quarter + j - 6)
    pick = (k == want).astype(F32)
    out[...] = lax.dot_general(
        pick, total[...], (((1,), (0,)), ((), ())), precision=lax.Precision.HIGHEST, preferred_element_type=F32
    )


def finish_kernel(parts, down, up, gain, tokens):
    heads = parts.shape[0]
    factor = tokens / parts[0, 7:8, 0:1]
    flip = 2 * lax.axis_index("dp") // lax.axis_size("dp")
    for s in range(heads):
        b = parts[s // 2 * 2 + (s + 2 * s // heads + flip) % 2] * factor
        up[:, s * HD : (s + 1) * HD] = b[0:2]
        down[:, s * HD : (s + 1) * HD] = b[2:4]
        gain[:, s * HD : (s + 1) * HD] = b[6:7]
    for t in range(heads // 4):
        b = parts[4 * t] + parts[4 * t + 1] + parts[4 * t + 2] + parts[4 * t + 3]
        down[:, (heads + t) * HD : (heads + t + 1) * HD] = b[4:6] * factor


VMEM = pl.BlockSpec(memory_space=pltpu.VMEM)


def within(mib):
    return pltpu.CompilerParams(vmem_limit_bytes=mib * 2**20)


def gather_ranks(adapter_lowering, adapter_raising, dp, seq, member, small):
    own = jnp.concatenate([adapter_lowering, adapter_raising], axis=2)
    cut = own.shape[2] // 2
    part = (member + lax.axis_index("dp") // 2) % 2
    own = jnp.where(part == 0, own[:, :, :cut], own[:, :, cut:])
    near = lax.ppermute(own, "dp", [(d, d ^ 1) for d in range(dp)])
    pair = jnp.concatenate([own, near], axis=0)
    pair, small = lax.optimization_barrier((pair, small))
    rings = [
        [(2 * z + hi) * seq + chip + (first + z) % 2 for z in range(dp // 2)]
        for hi in range(2)
        for chip in range(0, seq, 2)
        for first in range(2)
    ]
    half = lax.all_gather(pair, ("dp", "seq"), axis=0, tiled=True, axis_index_groups=rings)
    half = half.reshape(dp * own.shape[1], cut)
    other = lax.ppermute(half, "seq", [(s, s ^ 1) for s in range(seq)])
    return half, other, small


def shards(projections, rotated_query_gradient, gains, adapter_lowering, adapter_raising, activations, positions, valid):
    dp, seq = lax.axis_size("dp"), lax.axis_size("seq")
    proj, act = projections[0, 0], activations[0]
    tokens, features = proj.shape
    ranks = dp * adapter_lowering.shape[1]
    member = lax.axis_index("seq")
    tg = rotated_query_gradient.reshape(seq, tokens, HD)
    tg = lax.all_to_all(tg, "seq", 0, 0, tiled=True)
    tables = pl.pallas_call(
        inverse_kernel,
        out_shape=(jax.ShapeDtypeStruct((tokens, HD), F32),) * 3,
        in_specs=[VMEM] * 3,
        out_specs=(VMEM,) * 3,
        compiler_params=within(3),
    )(proj, *rope_tables(positions[:, 0], valid[0]))
    half, other, tables = gather_ranks(adapter_lowering, adapter_raising, dp, seq, member, tables)
    rows = ranks + REM
    delta, gain = pl.pallas_call(
        delta_kernel,
        out_shape=(
            jax.ShapeDtypeStruct((tokens, features), BF16),
            jax.ShapeDtypeStruct((seq, 8, HD), F32),
        ),
        in_specs=[VMEM] * 6,
        out_specs=(VMEM, VMEM),
        compiler_params=within(6),
        scratch_shapes=[pltpu.VMEM((8, features), F32)],
    )(tg, proj, *tables, gains)
    mine, theirs = pl.pallas_call(
        sums_kernel,
        out_shape=(
            jax.ShapeDtypeStruct((seq, rows, HD), F32),
            jax.ShapeDtypeStruct((seq, rows, HD), BF16),
        ),
        in_specs=[VMEM] * 6,
        out_specs=(VMEM, VMEM),
        compiler_params=within(8),
        scratch_shapes=[pltpu.VMEM((ranks, act.shape[1] + features), BF16)],
    )(act, half, other, delta, gain, valid)
    partner = lax.ppermute(theirs, "seq", [(s, s ^ 1) for s in range(seq)])
    both = (mine + partner.astype(F32)).astype(BF16)
    length = dp // 2
    at = [[[0, 0] for _ in range(seq // 2)] for _ in range(dp)]
    for d in range(dp):
        for m in range(seq):
            at[d][m // 2][parity(d, m, dp, seq)] = d * seq + m
    planes = [
        [at[2 * z + x][i][c] for x in range(2) for i in range(seq // 2)] for z in range(length) for c in range(2)
    ]
    blocks = lax.all_to_all(both, ("dp", "seq"), 0, 0, tiled=True, axis_index_groups=planes)
    rank_rows = pl.pallas_call(
        lambda *refs: spread_kernel(*refs, ranks=ranks // 2, length=length),
        out_shape=jax.ShapeDtypeStruct((8 * length, HD), F32),
        in_specs=[VMEM],
        out_specs=VMEM,
        compiler_params=within(4),
        scratch_shapes=[pltpu.VMEM((128, HD), F32)],
    )(blocks)
    along_z = [
        [at[2 * z + hi][i][c] for z in range(length)] for hi in range(2) for i in range(seq // 2) for c in range(2)
    ]
    shares = rank_rows.reshape(length, 8, HD)
    shares = lax.all_to_all(shares, ("dp", "seq"), 0, 0, tiled=True, axis_index_groups=along_z)
    share = jnp.sum(shares, axis=0)
    parts = lax.all_to_all(jnp.broadcast_to(share, (seq, 8, HD)), "seq", 0, 0, tiled=True)
    down, up, gain = pl.pallas_call(
        lambda *refs: finish_kernel(*refs, tokens=float(dp * seq * tokens)),
        out_shape=(
            jax.ShapeDtypeStruct((2, act.shape[1]), F32),
            jax.ShapeDtypeStruct((2, features), F32),
            jax.ShapeDtypeStruct((1, features), F32),
        ),
        in_specs=[VMEM],
        out_specs=(VMEM, VMEM, VMEM),
        compiler_params=within(4),
    )(parts)
    return down[None], up[None], gain


def solution(mesh):
    in_specs = (
        P(None, "dp", "seq", None),
        P(None, "dp", None, "seq"),
        P(),
        P(None, "dp", None),
        P(None, "dp", None),
        P("dp", "seq", None),
        P(None, "dp", "seq"),
        P("dp", "seq"),
    )
    out_specs = (P(None, "dp", None), P(None, "dp", None), P())
    return jax.shard_map(shards, mesh=mesh, in_specs=in_specs, out_specs=out_specs, check_vma=False)
```

```python
import jax
import jax.numpy as jnp
import numpy as np
from jax import lax
from jax.experimental import pallas as pl
from jax.experimental.pallas import tpu as pltpu
from jax.sharding import PartitionSpec as P


HD = 128
EPSILON = 1e-06
F32 = jnp.float32
BF16 = jnp.bfloat16

REM = 8


def onto(shape, dim):
    return lax.broadcasted_iota(jnp.int32, shape, dim)


def parity(video, member, dp, seq):
    return (member + 2 * member // seq + 2 * video // dp) % 2


def own_parity():
    return parity(lax.axis_index("dp"), lax.axis_index("seq"), lax.axis_size("dp"), lax.axis_size("seq"))


def nt(a, b):
    return lax.dot_general(a, b, (((1,), (1,)), ((), ())), preferred_element_type=F32)


def nn(a, b):
    return lax.dot_general(a, b, (((1,), (0,)), ((), ())), preferred_element_type=F32)


def rope_tables(positions, valid):
    one_sixth = HD // 6
    counts = (HD // 2 - 2 * one_sixth, one_sixth, one_sixth)
    group = np.repeat(np.concatenate([np.full(n, k) for k, n in enumerate(counts)]), 2)
    powers = np.concatenate([-np.arange(n) / n for n in counts])
    frequency = np.repeat((10000.0**powers).astype(np.float32), 2)
    sign = np.where(np.arange(HD) % 2 == 0, 1.0, -1.0).astype(np.float32)
    at = positions.astype(F32)
    index = jnp.where(group == 0, at[0][:, None], jnp.where(group == 1, at[1][:, None], at[2][:, None]))
    angles = index * frequency
    keep = valid.astype(F32)[:, None]
    return jnp.cos(angles) * keep, jnp.sin(angles) * (keep * sign)


def mean_of(parts, features):
    mean = jnp.sum((parts[0] + parts[1]) + (parts[2] + parts[3]), axis=1, keepdims=True) / features
    return jnp.broadcast_to(mean, (8, HD))


def inverse_kernel(proj, cosine, sine, cos, sin, square):
    tokens, features = proj.shape

    def eight(k, _):
        rows = pl.ds(pl.multiple_of(8 * k, 8), 8)
        acc = [jnp.zeros((8, HD), F32)] * 4
        for h in range(features // HD):
            p = proj[rows, h * HD : (h + 1) * HD].astype(F32)
            acc[h % 4] = acc[h % 4] + p * p
        inverse = lax.rsqrt(mean_of(acc, features) + EPSILON)
        cos[rows, :] = cosine[rows, :] * inverse
        sin[rows, :] = sine[rows, :] * inverse
        square[rows, :] = inverse * inverse
        return 0

    lax.fori_loop(0, tokens // 8, eight, 0, unroll=4)


def delta_kernel(tg, proj, cos, sin, square, gains, delta, gain, gains8):
    heads, tokens, _ = tg.shape
    features = heads * HD
    even = onto((8, HD), 1) % 2 == 0
    gain[...] = jnp.zeros_like(gain)
    gains8[...] = jnp.broadcast_to(gains[...], gains8.shape)
    group = 4

    def some(k, _):
        rows = [pl.ds(pl.multiple_of(8 * (group * k + b), 8), 8) for b in range(group)]
        ps = [[proj[r, h * HD : (h + 1) * HD].astype(F32) for h in range(heads)] for r in rows]
        turns = [(cos[r, :], sin[r, :]) for r in rows]
        ws = [[None] * heads for _ in rows]
        acc = [[jnp.zeros((8, HD), F32)] * 4 for _ in rows]
        for h in range(heads):
            gh = gains8[:, h * HD : (h + 1) * HD]
            total = gain[h]
            for b, r in enumerate(rows):
                g = tg[h, r, :].astype(F32)
                turned = jnp.where(even, pltpu.roll(g, HD - 1, 1), pltpu.roll(g, 1, 1))
                u = turns[b][0] * g + turns[b][1] * turned
                p = ps[b][h]
                total = total + u * p
                ws[b][h] = u * gh
                acc[b][h % 4] = acc[b][h % 4] + ws[b][h] * p
            gain[h] = total
        for b, r in enumerate(rows):
            mean = mean_of(acc[b], features) * square[r, :]
            for h in range(heads):
                delta[r, h * HD : (h + 1) * HD] = (ws[b][h] - ps[b][h] * mean).astype(BF16)
        return 0

    lax.fori_loop(0, tokens // (8 * group), some, 0)


def sums_kernel(act, half, other, delta, gain, valid, mine, theirs, maps):
    heads = gain.shape[0]
    ranks, cut = half.shape
    width = act.shape[1]
    each, quarter = ranks // 2, ranks // 8
    c, hi = own_parity(), lax.axis_index("dp") % 2
    part = (lax.axis_index("seq") + lax.axis_index("dp") // 2 + lax.axis_index("dp")) % 2

    @pl.when(part == 0)
    def _():
        maps[:, 0:cut] = half[...]
        maps[:, cut:] = other[...]

    @pl.when(part != 0)
    def _():
        maps[:, 0:cut] = other[...]
        maps[:, cut:] = half[...]

    def lanes(tile, count=1):
        return pl.ds(pl.multiple_of(tile * HD, HD), count * HD)

    r, k = onto((ranks, ranks), 0), onto((ranks, ranks), 1)
    far = (r >= each).astype(jnp.int32)
    loc = r - each * far
    order = (k == 2 * loc - (loc & 1) + 2 * (far ^ hi)).astype(F32).astype(BF16)
    up = nt(maps[:, 0:width], act[...]).astype(BF16)
    back = nt(maps[:, width:], delta[...]).astype(BF16)
    up = nn(order, up).astype(BF16)
    back = nn(order, back).astype(BF16)
    r, k = onto((8 * REM, ranks), 0), onto((8 * REM, ranks), 1)
    at = ((r >> 3) & 1) * each + (r >> 4) * quarter + (r & 7)
    pick = ((k == at) & ((r & 7) < quarter)).astype(F32).astype(BF16)
    rems = nn(pick, back).astype(BF16)
    count = jnp.sum(valid[...].astype(F32))
    row = onto((REM, HD), 0)

    def four(t, _):
        ups = nn(up, delta[:, lanes(4 * t, 4)])
        downs = nn(back, act[:, lanes(4 * t, 4)])
        rests = nn(rems, act[:, lanes(heads + t)])
        for p in range(2):
            i = 2 * t + p
            for x in range(2):
                pieces = []
                for q in (2 * p, 2 * p + 1):
                    cols, rows = slice(q * HD, (q + 1) * HD), slice(x * each, (x + 1) * each)
                    g = jnp.sum(gain[4 * t + q], axis=0, keepdims=True)
                    first = (2 * q + x) * REM
                    rest = rests[first : first + REM]
                    rest = jnp.where(row == quarter, g, jnp.where(row == quarter + 1, count, rest))
                    pieces.append((ups[rows, cols], downs[rows, cols], rest))
                for j, (top, size) in enumerate(((0, each), (each, each), (2 * each, REM))):
                    even, odd = pieces[0][j], pieces[1][j]
                    at = 2 * i + x
                    mine[at, top : top + size, :] = jnp.where(c == 0, even, odd)
                    theirs[at, top : top + size, :] = jnp.where(c == 0, odd, even).astype(theirs.dtype)
        return 0

    lax.fori_loop(0, heads // 4, four, 0, unroll=8)


def spread_kernel(blocks, out, total, ranks, length):
    peers, rows, _ = blocks.shape
    acc = blocks[0].astype(F32)
    for i in range(1, peers):
        acc = acc + blocks[i].astype(F32)
    total[...] = jnp.zeros_like(total)
    total[0:rows, :] = acc
    q = lax.axis_index("seq") // 2 % 2 * 2 + own_parity()
    quarter = ranks // 4
    shape = (8 * length, total.shape[0])
    r, k = onto(shape, 0), onto(shape, 1)
    j = r & 7
    at = 2 * (r >> 3) + (j & 1)
    want = jnp.where(j < 2, at, at + ranks)
    rem = at - quarter * q
    rem = jnp.where((rem >= 0) & (rem < quarter), 2 * ranks + rem, -1)
    want = jnp.where(j < 4, want, rem)
    want = jnp.where(j < 6, want, 2 * ranks + quarter + j - 6)
    pick = (k == want).astype(F32)
    out[...] = lax.dot_general(
        pick, total[...], (((1,), (0,)), ((), ())), precision=lax.Precision.HIGHEST, preferred_element_type=F32
    )


def finish_kernel(parts, down, up, gain, tokens):
    heads = parts.shape[0]
    factor = tokens / parts[0, 7:8, 0:1]
    flip = 2 * lax.axis_index("dp") // lax.axis_size("dp")
    for s in range(heads):
        b = parts[s // 2 * 2 + (s + 2 * s // heads + flip) % 2] * factor
        up[:, s * HD : (s + 1) * HD] = b[0:2]
        down[:, s * HD : (s + 1) * HD] = b[2:4]
        gain[:, s * HD : (s + 1) * HD] = b[6:7]
    for t in range(heads // 4):
        b = parts[4 * t] + parts[4 * t + 1] + parts[4 * t + 2] + parts[4 * t + 3]
        down[:, (heads + t) * HD : (heads + t + 1) * HD] = b[4:6] * factor


VMEM = pl.BlockSpec(memory_space=pltpu.VMEM)


def within(mib):
    return pltpu.CompilerParams(vmem_limit_bytes=mib * 2**20)


def gather_ranks(adapter_lowering, adapter_raising, dp, seq, member, small):
    own = jnp.concatenate([adapter_lowering, adapter_raising], axis=2)
    cut = own.shape[2] // 2
    video = lax.axis_index("dp")
    part = (member + video // 2 + video) % 2
    own = jnp.where(part == 0, own[:, :, :cut], own[:, :, cut:])
    moves = [(d * seq + m, (d ^ 1) * seq + (m ^ 1)) for d in range(dp) for m in range(seq)]
    near = lax.ppermute(own, ("dp", "seq"), moves)
    pair = jnp.concatenate([own, near], axis=0)
    pair, small = lax.optimization_barrier((pair, small))
    rings = [
        [(2 * z + hi) * seq + chip + (first + z) % 2 for z in range(dp // 2)]
        for hi in range(2)
        for chip in range(0, seq, 2)
        for first in range(2)
    ]
    half = lax.all_gather(pair, ("dp", "seq"), axis=0, tiled=True, axis_index_groups=rings)
    half = half.reshape(dp * own.shape[1], cut)
    other = lax.ppermute(half, "seq", [(s, s ^ 1) for s in range(seq)])
    return half, other, small


def shards(projections, rotated_query_gradient, gains, adapter_lowering, adapter_raising, activations, positions, valid):
    dp, seq = lax.axis_size("dp"), lax.axis_size("seq")
    proj, act = projections[0, 0], activations[0]
    tokens, features = proj.shape
    ranks = dp * adapter_lowering.shape[1]
    member = lax.axis_index("seq")
    tg = rotated_query_gradient.reshape(seq, tokens, HD)
    tg = lax.all_to_all(tg, "seq", 0, 0, tiled=True)
    tables = pl.pallas_call(
        inverse_kernel,
        out_shape=(jax.ShapeDtypeStruct((tokens, HD), F32),) * 3,
        in_specs=[VMEM] * 3,
        out_specs=(VMEM,) * 3,
        compiler_params=within(3),
    )(proj, *rope_tables(positions[:, 0], valid[0]))
    half, other, tables = gather_ranks(adapter_lowering, adapter_raising, dp, seq, member, tables)
    rows = ranks + REM
    delta, gain = pl.pallas_call(
        delta_kernel,
        out_shape=(
            jax.ShapeDtypeStruct((tokens, features), BF16),
            jax.ShapeDtypeStruct((seq, 8, HD), F32),
        ),
        in_specs=[VMEM] * 6,
        out_specs=(VMEM, VMEM),
        compiler_params=within(6),
        scratch_shapes=[pltpu.VMEM((8, features), F32)],
    )(tg, proj, *tables, gains)
    mine, theirs = pl.pallas_call(
        sums_kernel,
        out_shape=(
            jax.ShapeDtypeStruct((seq, rows, HD), F32),
            jax.ShapeDtypeStruct((seq, rows, HD), BF16),
        ),
        in_specs=[VMEM] * 6,
        out_specs=(VMEM, VMEM),
        compiler_params=within(8),
        scratch_shapes=[pltpu.VMEM((ranks, act.shape[1] + features), BF16)],
    )(act, half, other, delta, gain, valid)
    partner = lax.ppermute(theirs, "seq", [(s, s ^ 1) for s in range(seq)])
    both = (mine + partner.astype(F32)).astype(BF16)
    length = dp // 2
    at = [[[0, 0] for _ in range(seq // 2)] for _ in range(dp)]
    for d in range(dp):
        for m in range(seq):
            at[d][m // 2][parity(d, m, dp, seq)] = d * seq + m
    planes = [
        [at[2 * z + x][i][c] for i in range(seq // 2) for x in range(2)] for z in range(length) for c in range(2)
    ]
    blocks = lax.all_to_all(both, ("dp", "seq"), 0, 0, tiled=True, axis_index_groups=planes)
    rank_rows = pl.pallas_call(
        lambda *refs: spread_kernel(*refs, ranks=ranks // 2, length=length),
        out_shape=jax.ShapeDtypeStruct((8 * length, HD), F32),
        in_specs=[VMEM],
        out_specs=VMEM,
        compiler_params=within(4),
        scratch_shapes=[pltpu.VMEM((128, HD), F32)],
    )(blocks)
    along_z = [
        [at[2 * z + hi][i][c] for z in range(length)] for hi in range(2) for i in range(seq // 2) for c in range(2)
    ]
    shares = rank_rows.reshape(length, 8, HD)
    shares = lax.all_to_all(shares, ("dp", "seq"), 0, 0, tiled=True, axis_index_groups=along_z)
    share = jnp.sum(shares, axis=0)
    parts = lax.all_to_all(jnp.broadcast_to(share, (seq, 8, HD)), "seq", 0, 0, tiled=True)
    down, up, gain = pl.pallas_call(
        lambda *refs: finish_kernel(*refs, tokens=float(dp * seq * tokens)),
        out_shape=(
            jax.ShapeDtypeStruct((2, act.shape[1]), F32),
            jax.ShapeDtypeStruct((2, features), F32),
            jax.ShapeDtypeStruct((1, features), F32),
        ),
        in_specs=[VMEM],
        out_specs=(VMEM, VMEM, VMEM),
        compiler_params=within(4),
    )(parts)
    return down[None], up[None], gain


def solution(mesh):
    in_specs = (
        P(None, "dp", "seq", None),
        P(None, "dp", None, "seq"),
        P(),
        P(None, "dp", None),
        P(None, "dp", None),
        P("dp", "seq", None),
        P(None, "dp", "seq"),
        P("dp", "seq"),
    )
    out_specs = (P(None, "dp", None), P(None, "dp", None), P())
    return jax.shard_map(shards, mesh=mesh, in_specs=in_specs, out_specs=out_specs, check_vma=False)
```
